256 devices in a mesh: section: 16 (over z, x_hi), tensor: 16 (over x_lo, y, core).
Axes of the slice: x: 4 (x_hi: 2, x_lo: 2; x = x_hi * 2 + x_lo), y: 4, z: 8, core: 2. Of those that a mesh axis runs over, the one named last changes fastest.
Arguments:
- noise: float32 [2, 4, 32, 32], P(None, None, 'tensor'), may hold values from -6 to 6
- target: float32 [2, 4, 32, 32], P(None, None, 'tensor'), may hold values from -6 to 6
- timesteps: int32 [16], replicated, may hold values from 1 to 320, as said below
- w_in: float32 [4, 320], replicated, may hold values from -3 to 3
- gn_gain: float32 [320], replicated, may hold values from 0.1 to 1.9
- w_time1: float32 [320, 1280], replicated, may hold values from -0.3125 to 0.3125
- w_time2: float32 [1280, 320], replicated, may hold values from -0.15625 to 0.15625
- w_conv: bfloat16 [9, 320, 320], replicated, may hold values from -0.109375 to 0.109375
- w_out: float32 [320, 4], replicated, may hold values from -0.3125 to 0.3125
Outputs:
- trajectory: float32 [16, 2, 4, 32, 32], P('section', None, None, 'tensor')
- grad_conv: float32 [9, 320, 320], P(None, None, 'tensor')
The draws below stay inside these ranges and needn't reach their ends.
Inputs may be any that keep to these rules, and one draw needn't show every extreme that they name: `timesteps`: 16 distinct plan indices, strictly falling from one step to the next.
All inputs are finite; a program needn't handle non-finite values.
Results may differ from the reference program's by a relative error of at most 0.0008.
Values sent between devices are 32-bit elements; how exact they have to be, the bound alone decides.
No kernel may reach another device: no remote copies, remote signals or barrier semaphores. Data moves between devices by JAX's collectives and lax.ppermute only.
A program may use at most 64 MiB of HBM per device.

```python
import math
import jax
import jax.numpy as jnp
from jax import lax

C = 320
TEMB = 1280
GROUPS = 32
CHAN_IN = 4
WIDTH = 32
MICRO = 2
STEPS = 16
H = 32


def draw_timesteps(key, part):
    picked = jax.random.permutation(key, 20 * STEPS)[:STEPS] + 1
    return (-jnp.sort(-picked)).astype(jnp.int32)


def shard_levels(own_key, dims, shards, low, largest):
    gain, own = 1.0, jax.random.fold_in(own_key, 6)
    for position, parts in shards:
        heights = jnp.exp(jax.random.uniform(jax.random.fold_in(own, position), (parts,), jnp.float32, low / len(shards), largest / len(shards)))
        gain = gain * jnp.repeat(heights, dims[position] // parts).reshape([-1 if axis == position else 1 for axis in range(len(dims))])
    return gain


def centred(own_key, extent, spread, limit, split=(), kind=jnp.bfloat16):
    result = jax.random.normal(own_key, extent, jnp.float32) * spread
    if len(split) > 0:
        result = shard_levels(own_key, extent, split, -0.22, 0.18) * result
    return jnp.clip(result, min=-limit, max=limit).astype(kind)


def setup_inputs(seed: int = 0) -> dict:
    arg_keys = jax.random.split(jax.random.key(seed), 10)
    return {
        "noise": centred(arg_keys[0], (MICRO, CHAN_IN, H, WIDTH), 1.0, 6.0, ((2, 16),), jnp.float32),
        "target": centred(arg_keys[1], (MICRO, CHAN_IN, H, WIDTH), 1.0, 6.0, ((2, 16),), jnp.float32),
        "timesteps": draw_timesteps(jax.random.fold_in(arg_keys[9], 71), 0),
        "w_in": centred(arg_keys[3], (CHAN_IN, C), CHAN_IN ** -0.5, 3.0, (), jnp.float32),
        "gn_gain": jnp.clip(1.0 + 0.18 * jax.random.normal(arg_keys[4], (C,), jnp.float32), 0.1, 1.9),
        "w_time1": centred(arg_keys[5], (C, TEMB), C ** -0.5, 0.3125, (), jnp.float32),
        "w_time2": centred(arg_keys[6], (TEMB, C), TEMB ** -0.5, 0.15625, (), jnp.float32),
        "w_conv": centred(arg_keys[7], (9, C, C), (9 * C) ** -0.5, 0.109375),
        "w_out": centred(arg_keys[8], (C, CHAN_IN), C ** -0.5, 0.3125, (), jnp.float32),
    }


precise = lax.Precision.HIGHEST

def alpha_table():
    step_grid = jnp.arange(1000, dtype=jnp.float32)
    lowest = jnp.sqrt(jnp.asarray(0.00085, jnp.float32))
    highest = jnp.sqrt(jnp.asarray(0.012, jnp.float32))
    betas = (lowest + step_grid * ((highest - lowest) / 999.0)) ** 2
    return jnp.cumprod(1.0 - betas)

def section_terms(timesteps, section_index, alphas, w_time1, w_time2, features):
    positions = jnp.arange(timesteps.shape[0], dtype=jnp.int32)
    current = jnp.sum(jnp.where(positions == section_index, timesteps, 0))
    following = jnp.sum(jnp.where(positions == section_index + 1, timesteps, 0))
    step_grid = jnp.arange(alphas.shape[0], dtype=jnp.int32)
    alpha_now = jnp.sum(jnp.where(step_grid == current, alphas, 0.0))
    alpha_next = jnp.where(section_index + 1 < timesteps.shape[0], jnp.sum(jnp.where(step_grid == following, alphas, 0.0)), 1.0)
    keep_coef = jnp.sqrt(alpha_next / alpha_now)
    noise_coef = jnp.sqrt(1.0 - alpha_next) - keep_coef * jnp.sqrt(1.0 - alpha_now)
    half_width = features // 2
    frequency = jnp.exp(-math.log(10000.0) * jnp.arange(half_width, dtype=jnp.float32) / half_width)
    angles = current.astype(jnp.float32) * frequency
    sinusoid = jnp.concatenate([jnp.cos(angles), jnp.sin(angles)])
    hidden = jax.nn.silu(jnp.dot(sinusoid, w_time1, precision=precise))
    return (keep_coef, noise_coef, jnp.dot(hidden, w_time2, precision=precise))

def group_partial(latent, w_in, groups):
    projected = jnp.einsum('crw,cd->rwd', latent, w_in, precision=precise)
    grouped = projected.reshape(-1, groups, projected.shape[2] // groups)
    return (lax.optimization_barrier(jnp.sum(grouped, axis=(0, 2))), lax.optimization_barrier(jnp.sum(grouped * grouped, axis=(0, 2))))

def denoise_rows(latent_pad, row_mask, group_sum, squares, w_in, gn_gain, conv_weight, w_out, embed, keep_coef, noise_coef, count_all):
    projected = jnp.einsum('crw,cd->rwd', latent_pad, w_in, precision=precise)
    groups = group_sum.shape[0]
    features = projected.shape[2]
    group_avg = group_sum / count_all
    group_var = squares / count_all - group_avg * group_avg
    average = jnp.repeat(group_avg, features // groups)
    variance = jnp.repeat(group_var, features // groups)
    activated = jax.nn.silu((projected - average) * lax.rsqrt(variance + 1e-05) * gn_gain) * row_mask[:, None, None]
    activated = activated + lax.stop_gradient(activated.astype(jnp.bfloat16).astype(jnp.float32) - activated)
    activated = jnp.pad(activated, ((0, 0), (1, 1), (0, 0)))
    row_count = latent_pad.shape[1] - 2
    col_count = latent_pad.shape[2]
    convolved = jnp.zeros((row_count, col_count, features), jnp.float32)
    for offset in range(9):
        shift_row = offset // 3
        shift_col = offset % 3
        window = activated[shift_row:shift_row + row_count, shift_col:shift_col + col_count]
        convolved = convolved + jnp.einsum('rwc,cd->rwd', window, conv_weight[offset], precision=precise)
    hidden = projected[1:-1] + convolved + embed
    guess = jnp.einsum('rwd,dc->crw', hidden, w_out, precision=precise)
    return keep_coef * latent_pad[:, 1:-1] + noise_coef * guess

def reference(noise, target, timesteps, w_in, gn_gain, w_time1, w_time2, w_conv, w_out):
    alphas = alpha_table()
    micro_count, channels, height, breadth = noise.shape
    features = w_in.shape[1]
    count_all = jnp.asarray(height * breadth * (features // GROUPS), jnp.float32)
    row_mask = jnp.pad(jnp.ones((height,), jnp.float32), 1)
    section_ids = jnp.arange(STEPS, dtype=jnp.int32)

    def run_chain(conv_weight):

        def advance(latent, section_index):
            keep_coef, noise_coef, embed = section_terms(timesteps, section_index, alphas, w_time1, w_time2, features)
            group_sum, squares = group_partial(latent, w_in, GROUPS)
            latent_pad = jnp.pad(latent, ((0, 0), (1, 1), (0, 0)))
            stepped = denoise_rows(latent_pad, row_mask, group_sum, squares, w_in, gn_gain, conv_weight, w_out, embed, keep_coef, noise_coef, count_all)
            return (stepped, stepped)
        trajectories = []
        for micro_index in range(micro_count):
            _, steps_out = lax.scan(advance, noise[micro_index], section_ids)
            trajectories.append(steps_out)
        return jnp.stack(trajectories, axis=1)
    trajectory, pullback = jax.vjp(run_chain, w_conv.astype(jnp.float32))
    cotangent = jnp.zeros_like(trajectory).at[STEPS - 1].set(trajectory[STEPS - 1] - target)
    grad_conv = pullback(cotangent)[0]
    return (trajectory, grad_conv)
```

```python
import math

import jax
import jax.numpy as jnp
import numpy as np
from jax import lax
from jax.experimental import pallas as pl
from jax.experimental.pallas import tpu as pltpu
from jax.sharding import PartitionSpec as P


GROUPS = 32
STEPS = 16
CH = 4
C = 320
SIDE = 32
PIX = SIDE * SIDE
TILE = 256
F32 = jnp.float32
BF16 = jnp.bfloat16
EPS = 1e-05


def schedule_tables():
    grid = np.arange(1000, dtype=np.float64)
    low, high = math.sqrt(0.00085), math.sqrt(0.012)
    bar = np.cumprod(1.0 - (low + grid * ((high - low) / 999.0)) ** 2)
    table = np.zeros((3, 1024), np.float32)
    table[0, :1000] = np.sqrt(bar)
    table[1, :1000] = 1.0 / np.sqrt(bar)
    table[2, :1000] = np.sqrt(1.0 - bar)
    return table


def split(x, parts):
    out = []
    for _ in range(parts):
        head = x.astype(BF16)
        out.append(head)
        x = x - head.astype(F32)
    return out


def dot(a, b, dims=((1,), (0,)), precision=None):
    return lax.dot_general(a, b, (dims, ((), ())), precision=precision, preferred_element_type=F32)


NT = ((1,), (1,))


def rolled(x, shift, axis):
    return pltpu.roll(x, shift % x.shape[axis], axis)


def doubled(x):
    return jnp.concatenate([x, x], axis=0)


def row_index(shape):
    return lax.broadcasted_iota(jnp.int32, shape, 0)


def prepare_kernel(feat, w1, w2t, w_conv, w_out_t, w_in, w_fwd, w_bwd, emb, rows, cols):
    hi = lax.Precision.HIGHEST
    out8 = doubled(w_out_t[...])
    in8 = doubled(w_in[...])
    hidden = dot(feat[...], w1[...], precision=hi)
    hidden = hidden * jax.nn.sigmoid(hidden)
    embed = dot(hidden, w2t[...], NT, precision=hi)
    shift = dot(out8, embed, NT, precision=hi)
    for s in range(STEPS):
        emb[s] = jnp.broadcast_to(shift[:, s : s + 1], (8, 128))
    parts = split(out8, 3)
    stacked = jnp.concatenate([p.astype(F32) for p in parts] + [jnp.zeros_like(out8)], axis=0).astype(BF16)
    is_head = row_index((8, C)) < CH
    heads, tails, mixed = [], [], []
    for tap in range(9):
        got = dot(stacked, w_conv[tap], NT)
        full = got[0:8] + got[8:16] + got[16:24]
        head = full.astype(BF16).astype(F32)
        tail = full - head
        mixed.append(jnp.where(is_head, head, tail))
        heads.append(head)
        tails.append(tail)
    pad = jnp.zeros((8, C), F32)
    w_fwd[...] = jnp.concatenate(mixed + [pad], axis=0).astype(BF16)
    both = jnp.concatenate(heads + tails, axis=0)
    w_bwd[...] = both.T.astype(BF16)
    first = row_index((8, C)) < CH
    next1, next2 = rolled(in8, -1, 0), rolled(in8, -2, 0)
    top = jnp.where(first, in8, in8 * in8)
    low = in8 * jnp.where(first, 2.0 * next1, next2)
    a = lax.broadcasted_iota(jnp.int32, (C, C), 0) // (C // GROUPS)
    b = lax.broadcasted_iota(jnp.int32, (C, C), 1) // (C // GROUPS)
    member = (a == b).astype(F32)
    sums = dot(jnp.concatenate([top, low], axis=0), member, precision=hi)
    rows[...] = sums * (1.0 / (PIX * (C // GROUPS)))
    for j in range(CH):
        ahead = jnp.sum(out8 * rolled(in8, -j, 0), axis=1, keepdims=True)
        back = jnp.sum(rolled(out8, -j, 0) * in8, axis=1, keepdims=True)
        cols[j] = jnp.broadcast_to(ahead, (8, 128))
        cols[CH + j] = jnp.broadcast_to(back, (8, 128))


def prepare(feat, w1, w2t, w_conv, w_out_t, w_in):
    return pl.pallas_call(
        prepare_kernel,
        out_shape=(
            jax.ShapeDtypeStruct((80, C), BF16),
            jax.ShapeDtypeStruct((C, 144), BF16),
            jax.ShapeDtypeStruct((STEPS, 8, 128), F32),
            jax.ShapeDtypeStruct((16, C), F32),
            jax.ShapeDtypeStruct((8, 8, 128), F32),
        ),
        name="prepare",
    )(feat, w1, w2t, w_conv, w_out_t, w_in)


def wide(col):
    return jnp.concatenate([col] * (PIX // 128), axis=1)


def chain_kernel(
    place, times, table, recv, w_fwd, w_bwd, emb, rows, cols, gain, w_in,
    sent, lat, stat, act, slope, taps, total,
):
    section, block = place[0], place[1]
    rid = row_index((8, PIX))
    upper = rid < CH
    lane = lax.broadcasted_iota(jnp.int32, (8, PIX), 1)
    column = lane % SIDE
    not_left, not_right = column > 0, column < SIDE - 1
    not_top, not_bottom = lane >= SIDE, lane < PIX - SIDE
    srow = row_index((8, C))
    supper = srow < CH
    in8 = doubled(w_in[...])
    in5 = jnp.where(supper, in8, 0.0)
    half_gain = 0.5 * gain[...]

    start = jnp.concatenate([recv[i] for i in range(16)], axis=1)
    latent0 = jnp.where(upper, start, rolled(start, 4, 0))
    target8 = jnp.where(upper, rolled(start, 4, 0), start)

    def coefs(s):
        now = times[s]
        last = s == STEPS - 1
        after = times[jnp.minimum(s + 1, STEPS - 1)]
        root = jnp.where(last, 1.0, table[0, after])
        rest = jnp.where(last, 0.0, table[2, after])
        keep = root * table[1, now]
        return keep, rest - keep * table[2, now]

    def homogeneous(l8):
        return jnp.where(upper, l8, jnp.where(rid == CH, 1.0, 0.0))

    def forward(s, l8):
        keep, nc = coefs(s)
        lat[s] = l8
        r1, r2, r3 = rolled(l8, -1, 0), rolled(l8, -2, 0), rolled(l8, -3, 0)
        x0 = jnp.where(upper, l8, l8 * l8)
        x1 = l8 * jnp.where(upper, r1, r2)
        m0 = jnp.sum(x0, axis=1, keepdims=True)
        m1 = jnp.sum(x1, axis=1, keepdims=True)
        p0 = rows[0:8] * m0
        p1 = rows[8:16] * m1
        avg = jnp.sum(jnp.where(supper, p0, 0.0), axis=0, keepdims=True)
        sq = jnp.sum(jnp.where(supper, 0.0, p0) + p1, axis=0, keepdims=True)
        rstd = lax.rsqrt(sq - avg * avg + EPS)
        scale = rstd * half_gain
        stat[s, 0:1] = avg
        stat[s, 1:2] = rstd
        stat[s, 2:3] = scale
        wz = jnp.where(srow == CH, -avg * scale, in5 * scale)
        a, b, c = [p.astype(F32) for p in split(wz, 3)]
        wzs = jnp.concatenate([a, a, b, b, a, c], axis=0).T.astype(BF16)
        d, e, f = [p.astype(F32) for p in split(homogeneous(l8), 3)]
        ls = jnp.concatenate([d, e, d, e, f, d], axis=0).astype(BF16)
        linear = (
            wide(cols[0]) * l8 + wide(cols[1]) * r1 + wide(cols[2]) * r2 + wide(cols[3]) * r3
        )
        linear = keep * l8 + nc * (linear + wide(emb[s]))
        for j in range(PIX // TILE):
            at = slice(j * TILE, (j + 1) * TILE)
            h = dot(wzs, ls[:, at])
            t = jnp.tanh(h)
            u = h * t
            narrow = (h + u).astype(BF16)
            act[s, :, at] = narrow
            slope[s, :, at] = (1.0 + t) + (h - u * t)
            taps[:, at] = dot(w_fwd[...], narrow)

        def tap(dy, dx):
            k = 8 * (3 * dy + dx)
            return taps[k : k + 8]

        def column_sum(dx):
            above = jnp.where(not_top, rolled(tap(0, dx), SIDE, 1), 0.0)
            below = jnp.where(not_bottom, rolled(tap(2, dx), -SIDE, 1), 0.0)
            return tap(1, dx) + above + below

        conv = column_sum(1)
        conv = conv + jnp.where(not_left, rolled(column_sum(0), 1, 1), 0.0)
        conv = conv + jnp.where(not_right, rolled(column_sum(2), -1, 1), 0.0)
        conv = conv + rolled(conv, 4, 0)
        return linear + nc * conv

    final = lax.fori_loop(0, STEPS, forward, latent0)
    lat[STEPS] = final
    total[...] = jnp.zeros_like(total)

    def backward(i, adj):
        s = STEPS - 1 - i
        keep, nc = coefs(s)
        l8 = lat[s]
        avg, rstd, scale = stat[s, 0:1], stat[s, 1:2], stat[s, 2:3]
        ng = nc * adj
        head = ng.astype(BF16).astype(F32)
        x = jnp.where(upper, head, ng - head)
        shifted = []
        sides = (
            jnp.where(not_right, rolled(x, -1, 1), 0.0),
            x,
            jnp.where(not_left, rolled(x, 1, 1), 0.0),
        )
        for y in sides:
            shifted.append(jnp.where(not_bottom, rolled(y, -SIDE, 1), 0.0))
        shifted.extend(sides)
        for y in sides:
            shifted.append(jnp.where(not_top, rolled(y, SIDE, 1), 0.0))
        col = jnp.concatenate(shifted + shifted, axis=0).astype(BF16)
        ws = in8 * scale
        whead = ws.astype(BF16).astype(F32)
        wd = jnp.where(supper, whead, ws - whead).astype(BF16)
        d, e = [p.astype(F32) for p in split(homogeneous(l8), 2)]
        ls = jnp.concatenate([d, e], axis=0).astype(BF16)
        direct = []
        sx = jnp.zeros((16, C), F32)
        grad = jnp.zeros((72, C), F32)
        for j in range(PIX // TILE):
            at = slice(j * TILE, (j + 1) * TILE)
            g = dot(w_bwd[...], col[:, at]) * slope[s, :, at]
            g0, g1 = split(g, 2)
            direct.append(dot(wd, g0) + dot(wd, g1))
            sx = sx + dot(ls[:, at], g0, NT) + dot(ls[:, at], g1, NT)
            grad = grad + dot(col[:72, at], act[s, :, at], NT)
        total[...] += grad
        dl = jnp.concatenate(direct, axis=1)
        dl = dl + rolled(dl, 4, 0)
        sx = sx[0:8] + sx[8:16]
        s1 = sx[CH : CH + 1]
        lw = jnp.sum(in5 * sx, axis=0, keepdims=True)
        q = (-0.5 * rstd * rstd * rstd) * half_gain * (lw - avg * s1)
        da = -scale * s1 - 2.0 * avg * q
        c0 = jnp.sum(rows[0:8] * jnp.where(supper, da, q), axis=1, keepdims=True)
        c1 = jnp.sum(rows[8:16] * q, axis=1, keepdims=True)
        c0 = jnp.broadcast_to(c0, (8, 128))
        c1 = jnp.broadcast_to(c1, (8, 128))
        up8 = upper[:, :128]
        c0r, c1r = rolled(c0, 4, 0), rolled(c1, 4, 0)
        dm = jnp.where(up8, c0, c0r)
        d0 = 2.0 * jnp.where(up8, c0r, c0)
        d1 = jnp.where(up8, c1, c1r)
        d3 = rolled(d1, 1, 0)
        d2 = jnp.where(up8, c1r, c1)
        d2 = d2 + rolled(d2, 2, 0)
        r1, r2, r3 = rolled(l8, -1, 0), rolled(l8, -2, 0), rolled(l8, -3, 0)
        stats = wide(dm) + wide(d0) * l8 + wide(d1) * r1 + wide(d2) * r2 + wide(d3) * r3
        a1, a2, a3 = rolled(adj, -1, 0), rolled(adj, -2, 0), rolled(adj, -3, 0)
        linear = (
            wide(cols[4]) * adj + wide(cols[5]) * a1 + wide(cols[6]) * a2 + wide(cols[7]) * a3
        )
        return keep * adj + nc * linear + dl + stats

    lax.fori_loop(0, STEPS, backward, final - target8)
    for k in range(9):
        part = total[8 * k : 8 * k + 8]
        part = part + rolled(part, 4, 0)
        sent[4 * k : 4 * k + 4] = part[0:4]
    mine = lat[section + 1, :, pl.ds(pl.multiple_of(block * 128, 128), 128)]
    sent[36:40] = jnp.concatenate([mine[0:4], jnp.zeros((4, C - 128), F32)], axis=1)


def chain(place, times, table, recv, w_fwd, w_bwd, emb, rows, cols, gain, w_in):
    smem = pl.BlockSpec(memory_space=pltpu.SMEM)
    vmem = pl.BlockSpec(memory_space=pltpu.VMEM)
    return pl.pallas_call(
        chain_kernel,
        out_shape=jax.ShapeDtypeStruct((40, C), F32),
        in_specs=[smem] * 3 + [vmem] * 8,
        out_specs=vmem,
        scratch_shapes=[
            pltpu.VMEM((STEPS + 1, 8, PIX), F32),
            pltpu.VMEM((STEPS, 8, C), F32),
            pltpu.VMEM((STEPS, C, PIX), BF16),
            pltpu.VMEM((STEPS, C, PIX), F32),
            pltpu.VMEM((80, PIX), F32),
            pltpu.VMEM((72, C), F32),
        ],
        name="chain",
    )(place, times, table, recv, w_fwd, w_bwd, emb, rows, cols, gain, w_in)


def finish_kernel(place, own, other, w_out_t, path, grad):
    core = place[2]
    hi = lax.Precision.HIGHEST
    mine = own[36:40, 0:128]
    theirs = other[36:40, 0:128]
    first = jnp.where(core == 0, mine, rolled(theirs, 64, 1))
    second = jnp.where(core == 0, theirs, rolled(mine, 64, 1))
    for m, x in enumerate((first, second)):
        for c in range(CH):
            for r in range(2):
                path[0, m, c, r : r + 1] = x[c : c + 1, SIDE * r : SIDE * r + SIDE]
    both = own[0:36] + other[0:36]
    for k in range(9):
        grad[k] = dot(w_out_t[...], both[4 * k : 4 * k + 4], precision=hi)


def finish(place, own, other, w_out_rows):
    smem = pl.BlockSpec(memory_space=pltpu.SMEM)
    vmem = pl.BlockSpec(memory_space=pltpu.VMEM)
    width = w_out_rows.shape[0]
    return pl.pallas_call(
        finish_kernel,
        out_shape=(
            jax.ShapeDtypeStruct((1, 2, CH, 2, SIDE), F32),
            jax.ShapeDtypeStruct((9, width, C), F32),
        ),
        in_specs=[smem] + [vmem] * 3,
        out_specs=(vmem, vmem),
        name="finish",
    )(place, own, other, w_out_rows)


def features(times):
    half = C // 2
    frequency = jnp.exp(-math.log(10000.0) * jnp.arange(half, dtype=F32) / half)
    angles = times.astype(F32)[:, None] * frequency[None]
    return jnp.concatenate([jnp.cos(angles), jnp.sin(angles)], axis=1)


def local(noise, target, timesteps, w_in, gn_gain, w_time1, w_time2, w_conv, w_out):
    count = lax.axis_size("tensor")
    index = lax.axis_index("tensor")
    place = jnp.stack([lax.axis_index("section"), index // 2, index % 2]).astype(jnp.int32)
    both = jnp.concatenate([noise.reshape(2, CH, 2 * SIDE), target.reshape(2, CH, 2 * SIDE)], axis=1)
    packed = jnp.tile(both, (count // 2, 1, 1))
    recv = lax.all_to_all(packed, "tensor", 0, 0, tiled=True)
    w_out_t = w_out.T
    made = prepare(features(timesteps), w_time1, w_time2.T, w_conv, w_out_t, w_in)
    own = chain(place, timesteps, jnp.asarray(schedule_tables()), recv, *made, gn_gain[None], w_in)
    other = lax.ppermute(own, "tensor", [(i, i ^ 1) for i in range(count)])
    width = C // count
    share = lax.dynamic_slice_in_dim(w_out, index * width, width, axis=0)
    path, grad = finish(place, own, other, share)
    return path, jnp.swapaxes(grad, 1, 2)


def solution(mesh):
    placed = (
        P(None, None, "tensor", None),
        P(None, None, "tensor", None),
        P(),
        P(),
        P(),
        P(),
        P(),
        P(),
        P(),
    )
    return jax.shard_map(
        local,
        mesh=mesh,
        in_specs=placed,
        out_specs=(P("section", None, None, "tensor", None), P(None, None, "tensor")),
        check_vma=False,
    )
```

```python
import math

import jax
import jax.numpy as jnp
import numpy as np
from jax import lax
from jax.experimental import pallas as pl
from jax.experimental.pallas import tpu as pltpu
from jax.sharding import PartitionSpec as P


GROUPS = 32
STEPS = 16
CH = 4
C = 320
SIDE = 32
PIX = SIDE * SIDE
TILE = 256
F32 = jnp.float32
BF16 = jnp.bfloat16
EPS = 1e-05


def schedule_tables():
    grid = np.arange(1000, dtype=np.float64)
    low, high = math.sqrt(0.00085), math.sqrt(0.012)
    bar = np.cumprod(1.0 - (low + grid * ((high - low) / 999.0)) ** 2)
    table = np.zeros((3, 1024), np.float32)
    table[0, :1000] = np.sqrt(bar)
    table[1, :1000] = 1.0 / np.sqrt(bar)
    table[2, :1000] = np.sqrt(1.0 - bar)
    return table


def split(x, parts):
    out = []
    for _ in range(parts):
        head = x.astype(BF16)
        out.append(head)
        x = x - head.astype(F32)
    return out


def dot(a, b, dims=((1,), (0,)), precision=None):
    return lax.dot_general(a, b, (dims, ((), ())), precision=precision, preferred_element_type=F32)


NT = ((1,), (1,))


def rolled(x, shift, axis):
    return pltpu.roll(x, shift % x.shape[axis], axis)


def doubled(x):
    return jnp.concatenate([x, x], axis=0)


def row_index(shape):
    return lax.broadcasted_iota(jnp.int32, shape, 0)


def position():
    return lax.axis_index("section"), lax.axis_index("tensor")


def wave_tables():
    half = C // 2
    f = np.exp(-math.log(10000.0) * np.arange(half, dtype=np.float64) / half)
    step = np.arange(32, dtype=np.float64)[:, None]
    big, small = 32.0 * step * f, step * f
    both = lambda a, b: np.concatenate([a, b], axis=1)
    return np.stack(
        [
            both(np.cos(big), np.sin(big)),
            both(-np.sin(big), np.cos(big)),
            both(np.cos(small), np.cos(small)),
            both(np.sin(small), np.sin(small)),
        ]
    ).astype(np.float32)


def pack_kernel(noise, target, packed):
    for m in range(2):
        parts = [x[m, :, r, :] for x in (noise, target) for r in range(2)]
        tile = jnp.concatenate(parts, axis=1)
        for j in range(8):
            packed[2 * j + m] = tile


def pack(noise, target):
    vmem = pl.BlockSpec(memory_space=pltpu.VMEM)
    return pl.pallas_call(
        pack_kernel,
        out_shape=jax.ShapeDtypeStruct((16, CH, 128), F32),
        in_specs=[vmem] * 2,
        out_specs=vmem,
        name="pack",
    )(noise, target)


def two(x):
    head = x.astype(BF16)
    return head, (x - head.astype(F32)).astype(BF16)


def stacked(a, b):
    return jnp.concatenate([a.astype(F32), b.astype(F32)], axis=0).astype(BF16)


def prepare_kernel(
    times, waves, w_out_t, w_in, gain, w1_hbm, w2t_hbm, conv_hbm,
    w_fwd, w_bwd, emb, rows, cols, w1, w2t, conv, sems,
):
    copies = [pltpu.make_async_copy(conv_hbm.at[k], conv.at[k], sems.at[k]) for k in range(9)]
    copies.append(pltpu.make_async_copy(w1_hbm, w1, sems.at[9]))
    copies.append(pltpu.make_async_copy(w2t_hbm, w2t, sems.at[10]))
    for c in copies:
        c.start()
    out8 = doubled(w_out_t[...])
    in8 = doubled(w_in[...])
    first = row_index((8, C)) < CH
    next1, next2 = rolled(in8, -1, 0), rolled(in8, -2, 0)
    top = jnp.where(first, in8, in8 * in8)
    low = in8 * jnp.where(first, 2.0 * next1, next2)
    group = lambda axis: lax.broadcasted_iota(jnp.int32, (C, C), axis) * 6554 >> 16
    member = jnp.where(group(0) == group(1), 1.0, 0.0).astype(BF16)
    both = jnp.concatenate([top, low], axis=0)
    p1, p2, p3 = [p.astype(F32) for p in split(both, 3)]
    sums = dot(jnp.concatenate([p1, p2, p3], axis=0).astype(BF16), member)
    sums = (sums[0:16] + sums[16:32] + sums[32:48]) * (1.0 / (PIX * (C // GROUPS)))
    rows[0:16] = sums
    for c in range(CH):
        rows[16 * (c + 1) : 16 * (c + 2)] = sums * w_in[c : c + 1]
    rows[80:88] = jnp.broadcast_to(0.5 * gain[...].reshape(1, C), (8, C))
    for j in range(CH):
        ahead = jnp.sum(out8 * rolled(in8, -j, 0), axis=1, keepdims=True)
        back = jnp.sum(rolled(out8, -j, 0) * in8, axis=1, keepdims=True)
        cols[j] = jnp.broadcast_to(ahead, (8, 128))
        cols[CH + j] = jnp.broadcast_to(back, (8, 128))
    repeated = jnp.concatenate([out8] * 16, axis=0).T
    lane = lax.broadcasted_iota(jnp.int32, (C, 128), 1)
    r_head, r_tail = two(repeated)
    r_head, r_tail = r_head.astype(F32), r_tail.astype(F32)
    acc = jnp.zeros((C, 256), F32)
    for k in range(9):
        copies[k].wait()
    for k in range(9):
        at = lane // 8 == k
        right = jnp.concatenate([jnp.where(at, r_head, 0.0), jnp.where(at, r_tail, 0.0)], axis=1)
        acc = acc + dot(conv[k], right.astype(BF16))
    full = acc[:, :128] + acc[:, 128:]
    head = full.astype(BF16).astype(F32)
    tail = full - head
    w_bwd[...] = jnp.concatenate([head[:, :80], tail[:, :80]], axis=1).astype(BF16)
    w_fwd[...] = jnp.where(lane % 8 < CH, head, tail).T[:80].astype(BF16)
    feats = []
    for s in range(STEPS):
        t = times[s]
        a, b = t >> 5, t & 31
        feats.append(
            waves[0, pl.ds(a, 1)] * waves[2, pl.ds(b, 1)]
            + waves[1, pl.ds(a, 1)] * waves[3, pl.ds(b, 1)]
        )
    f_head, f_tail = two(jnp.concatenate(feats, axis=0))
    o_head, o_tail = two(out8)
    copies[9].wait()
    w_head, w_tail = two(w1[...])
    z = dot(stacked(f_head, f_tail), w_head)
    z = 0.5 * (z[:STEPS] + z[STEPS:] + dot(f_head, w_tail))
    hidden = z + z * jnp.tanh(z)
    copies[10].wait()
    w_head, w_tail = two(w2t[...])
    y = dot(stacked(o_head, o_tail), w_head)
    y = y[0:8] + y[8:16] + dot(o_head, w_tail)
    y_head, y_tail = two(y)
    h_head, h_tail = two(hidden)
    x = dot(stacked(y_head, y_tail), h_head, NT)
    shift = x[0:8] + x[8:16] + dot(y_head, h_tail, NT)
    for s in range(STEPS):
        emb[s] = jnp.broadcast_to(shift[:, s : s + 1], (8, 128))


def prepare(times, w_out_t, w_in, gain, w1, w2t, w_conv):
    smem = pl.BlockSpec(memory_space=pltpu.SMEM)
    vmem = pl.BlockSpec(memory_space=pltpu.VMEM)
    hbm = pl.BlockSpec(memory_space=pl.ANY)
    return pl.pallas_call(
        prepare_kernel,
        out_shape=(
            jax.ShapeDtypeStruct((80, C), BF16),
            jax.ShapeDtypeStruct((C, 160), BF16),
            jax.ShapeDtypeStruct((STEPS, 8, 128), F32),
            jax.ShapeDtypeStruct((88, C), F32),
            jax.ShapeDtypeStruct((8, 8, 128), F32),
        ),
        in_specs=[smem] + [vmem] * 4 + [hbm] * 3,
        out_specs=(vmem,) * 5,
        scratch_shapes=[
            pltpu.VMEM(w1.shape, F32),
            pltpu.VMEM(w2t.shape, F32),
            pltpu.VMEM(w_conv.shape, BF16),
            pltpu.SemaphoreType.DMA((11,)),
        ],
        name="prepare",
    )(times, jnp.asarray(wave_tables()), w_out_t, w_in, gain, w1, w2t, w_conv)


def wide(col):
    return jnp.concatenate([col] * (PIX // 128), axis=1)


def chain_kernel(
    times, table, recv, w_fwd, w_bwd, emb, rows, cols, w_in,
    sent, lat, stat, act, slope, taps, total,
):
    section, index = position()
    rid = row_index((8, PIX))
    upper = rid < CH
    lane = lax.broadcasted_iota(jnp.int32, (8, 128), 1)
    column = lane % SIDE
    col_ok = {1: column > 0, 0: None, -1: column < SIDE - 1}
    low_ok, high_ok = lane >= SIDE, lane < 128 - SIDE
    srow = row_index((8, C))
    supper = srow < CH
    in8 = doubled(w_in[...])
    in5 = jnp.where(supper, in8, 0.0)
    half_gain = rows[80:81]

    def piece(x, v):
        return x[:, 128 * v : 128 * v + 128]

    def moved(x, d):
        return x if d == 0 else jnp.where(col_ok[d], rolled(x, d, 1), 0.0)

    def moved_low(x, d):
        y = rolled(x, SIDE + d, 1)
        return jnp.where(low_ok if d == 0 else low_ok & col_ok[d], y, 0.0)

    def moved_high(x, d):
        y = rolled(x, d - SIDE, 1)
        return jnp.where(high_ok if d == 0 else high_ok & col_ok[d], y, 0.0)

    got = [recv[i] for i in range(16)]

    def gathered(base):
        parts = []
        for v in range(8):
            at = base + SIDE * (v % 2)
            parts.extend(got[(8 * q + v) // 2][:, at : at + SIDE] for q in range(4))
        return doubled(jnp.concatenate(parts, axis=1))

    latent0, target8 = gathered(0), gathered(2 * SIDE)

    def coefs(s):
        now = times[s]
        last = s == STEPS - 1
        after = times[jnp.minimum(s + 1, STEPS - 1)]
        root = jnp.where(last, 1.0, table[0, after])
        rest = jnp.where(last, 0.0, table[2, after])
        keep = root * table[1, now]
        return keep, rest - keep * table[2, now]

    def forward(s, l8):
        keep, nc = coefs(s)
        lat[s] = l8
        r1, r2, r3 = rolled(l8, -1, 0), rolled(l8, -2, 0), rolled(l8, -3, 0)
        x0 = jnp.where(upper, l8, l8 * l8)
        x1 = l8 * jnp.where(upper, r1, r2)
        m0 = jnp.sum(x0, axis=1, keepdims=True)
        m1 = jnp.sum(x1, axis=1, keepdims=True)
        p0 = rows[0:8] * m0
        p1 = rows[8:16] * m1
        avg = jnp.sum(jnp.where(supper, p0, 0.0), axis=0, keepdims=True)
        sq = jnp.sum(jnp.where(supper, 0.0, p0) + p1, axis=0, keepdims=True)
        rstd = lax.rsqrt(sq - avg * avg + EPS)
        scale = rstd * half_gain
        stat[s, 0:1] = avg
        stat[s, 1:2] = rstd
        stat[s, 2:3] = scale
        wz = jnp.where(srow == CH, -avg * scale, in5 * scale)
        a = wz.astype(BF16).astype(F32)
        wzs = jnp.concatenate([a, a, wz - a], axis=0).T.astype(BF16)
        hom = jnp.where(upper, l8, jnp.where(rid == CH, 1.0, 0.0))
        d = hom.astype(BF16).astype(F32)
        ls = jnp.concatenate([d, hom - d, d], axis=0).astype(BF16)
        linear = (
            wide(cols[0]) * l8 + wide(cols[1]) * r1 + wide(cols[2]) * r2 + wide(cols[3]) * r3
        )
        linear = keep * l8 + nc * (linear + wide(emb[s]))
        tiles = [slice(j * TILE, (j + 1) * TILE) for j in range(PIX // TILE)]
        hs = [dot(wzs, ls[:, at]) for at in tiles]
        for at, h in zip(tiles, hs):
            t = jnp.tanh(h)
            u = h * t
            narrow = (h + u).astype(BF16)
            act[s, :, at] = narrow
            taps[:, at] = dot(w_fwd[...], narrow)
            slope[s, :, at] = ((1.0 + t) + (h - u * t)).astype(BF16)

        def tap(dy, dx, v):
            k = 8 * (3 * dy + dx)
            return taps[k : k + 8, 128 * v : 128 * v + 128]

        out = []
        for v in range(8):
            conv = None
            for dx in (1, 0, 2):
                d = 1 - dx
                part = tap(1, dx, v)
                if v > 0:
                    part = part + tap(0, dx, v - 1)
                if v < 7:
                    part = part + tap(2, dx, v + 1)
                part = moved(part, d)
                conv = part if conv is None else conv + part
                if v == 0:
                    conv = conv + moved_low(tap(0, dx, 7), d)
                if v == 7:
                    conv = conv + moved_high(tap(2, dx, 0), d)
            conv = conv + rolled(conv, 4, 0)
            out.append(piece(linear, v) + nc * conv)
        return jnp.concatenate(out, axis=1)

    final = lax.fori_loop(0, STEPS, forward, latent0)
    lat[STEPS] = final
    total[...] = jnp.zeros_like(total)
    erow = row_index((16, C)) < CH

    def backward(i, adj):
        s = STEPS - 1 - i
        keep, nc = coefs(s)
        l8 = lat[s]
        avg, rstd, scale = stat[s, 0:1], stat[s, 1:2], stat[s, 2:3]
        ng = nc * adj
        head = ng.astype(BF16).astype(F32)
        x = jnp.where(upper, head, ng - head)
        first, last = piece(x, 0), piece(x, 7)
        above, same, below = [], [], []
        for d in (-1, 0, 1):
            ys = [moved(piece(x, v), d) for v in range(8)]
            same.append(jnp.concatenate(ys, axis=1))
            above.append(jnp.concatenate(ys[1:] + [moved_high(first, d)], axis=1))
            below.append(jnp.concatenate([moved_low(last, d)] + ys[:7], axis=1))
        pad = jnp.zeros_like(x)
        a80 = jnp.concatenate(above + same + below + [pad], axis=0).astype(BF16)
        col = jnp.concatenate([a80, a80], axis=0)
        ws = in8 * scale
        whead = ws.astype(BF16).astype(F32)
        wd = jnp.where(supper, whead, ws - whead)
        q = (-0.5 * rstd * rstd * rstd) * half_gain
        qa = q * avg
        per = jnp.where(erow, -2.0 * qa, q)
        one = jnp.where(erow, 2.0 * qa * avg - scale, -qa)
        phi = [rows[16 * (c + 1) : 16 * (c + 2)] * per for c in range(CH)]
        phi = jnp.concatenate(phi + [rows[0:16] * one, wd, jnp.zeros_like(wd)], axis=0).astype(BF16)
        tiles = [slice(j * TILE, (j + 1) * TILE) for j in range(PIX // TILE)]
        gs = [dot(w_bwd[...], col[:, at]) for at in tiles]
        outs = []
        for at, g in zip(tiles, gs):
            outs.append(dot(phi, g.astype(BF16) * slope[s, :, at]))
        total[...] += dot(act[s], a80, NT)
        z = jnp.concatenate(outs, axis=1)
        dl = z[80:88]
        dl = dl + rolled(dl, 4, 0)
        acc0, acc1 = z[64:72], z[72:80]
        for c in range(CH):
            lc = l8[c : c + 1]
            acc0 = acc0 + z[16 * c : 16 * c + 8] * lc
            acc1 = acc1 + z[16 * c + 8 : 16 * c + 16] * lc
        c0 = jnp.sum(acc0, axis=1, keepdims=True)
        c1 = jnp.sum(acc1, axis=1, keepdims=True)
        c0 = jnp.broadcast_to(c0, (8, 128))
        c1 = jnp.broadcast_to(c1, (8, 128))
        up8 = upper[:, :128]
        c0r, c1r = rolled(c0, 4, 0), rolled(c1, 4, 0)
        dm = jnp.where(up8, c0, c0r)
        d0 = 2.0 * jnp.where(up8, c0r, c0)
        d1 = jnp.where(up8, c1, c1r)
        d3 = rolled(d1, 1, 0)
        d2 = jnp.where(up8, c1r, c1)
        d2 = d2 + rolled(d2, 2, 0)
        r1, r2, r3 = rolled(l8, -1, 0), rolled(l8, -2, 0), rolled(l8, -3, 0)
        a1, a2, a3 = rolled(adj, -1, 0), rolled(adj, -2, 0), rolled(adj, -3, 0)
        linear = (
            wide(cols[4]) * adj + wide(cols[5]) * a1 + wide(cols[6]) * a2 + wide(cols[7]) * a3
        )
        linear = keep * adj + nc * linear + dl
        stats = wide(dm) + wide(d0) * l8 + wide(d1) * r1 + wide(d2) * r2 + wide(d3) * r3
        return linear + stats

    lax.fori_loop(0, STEPS, backward, final - target8)
    turned = total[...].T
    for k in range(9):
        part = turned[8 * k : 8 * k + 8]
        part = part + rolled(part, 4, 0)
        sent[4 * k : 4 * k + 4] = part[0:4]
    mine = lat[section + 1, :, pl.ds(pl.multiple_of(index % 4 // 2 * 512, 512), 512)]
    blank = jnp.zeros((4, C - 128), F32)
    for v in range(4):
        sent[36 + 4 * v : 40 + 4 * v] = jnp.concatenate([piece(mine, v)[0:4], blank], axis=1)


def chain(times, table, recv, w_fwd, w_bwd, emb, rows, cols, w_in):
    smem = pl.BlockSpec(memory_space=pltpu.SMEM)
    vmem = pl.BlockSpec(memory_space=pltpu.VMEM)
    return pl.pallas_call(
        chain_kernel,
        out_shape=jax.ShapeDtypeStruct((56, C), F32),
        in_specs=[smem] * 2 + [vmem] * 7,
        out_specs=vmem,
        scratch_shapes=[
            pltpu.VMEM((STEPS + 1, 8, PIX), F32),
            pltpu.VMEM((STEPS, 8, C), F32),
            pltpu.VMEM((STEPS, C, PIX), BF16),
            pltpu.VMEM((STEPS, C, PIX), BF16),
            pltpu.VMEM((80, PIX), F32),
            pltpu.VMEM((C, 80), F32),
        ],
        name="chain",
    )(times, table, recv, w_fwd, w_bwd, emb, rows, cols, w_in)


def finish_kernel(own, other, w_out_t, path, grad):
    index = position()[1]
    core, turn = index % 2, (128 - SIDE * (index // 4)) % 128
    for r in range(2):
        k = 36 + 4 * r
        mine = jnp.where(core == 0, own[k : k + 4, 0:128], own[k + 8 : k + 12, 0:128])
        theirs = jnp.where(core == 0, other[k : k + 4, 0:128], other[k + 8 : k + 12, 0:128])
        first = jnp.where(core == 0, mine, theirs)
        second = jnp.where(core == 0, theirs, mine)
        for m, x in enumerate((first, second)):
            x = pltpu.roll(x, turn, 1)
            for c in range(CH):
                path[0, m, c, r : r + 1] = x[c : c + 1, 0:SIDE]
    width = grad.shape[1]
    weights = jnp.concatenate([w_out_t[...], jnp.zeros((CH, 384 - C), F32)], axis=1)
    weights = pltpu.roll(weights, (384 - width * index) % 384, 1)[:, :128]
    w_head = weights.astype(BF16).astype(F32)
    left = jnp.concatenate([w_head, w_head, weights - w_head, weights * 0.0], axis=0)
    left = left.T[:24].astype(BF16)
    both = own[0:36] + other[0:36]
    head = both.astype(BF16).astype(F32)
    tail = both - head
    for k in range(9):
        at = slice(4 * k, 4 * k + 4)
        right = jnp.concatenate([head[at], tail[at], head[at], tail[at]], axis=0)
        grad[k] = dot(left, right.astype(BF16))[:width]


def finish(own, other, w_out_t, width):
    vmem = pl.BlockSpec(memory_space=pltpu.VMEM)
    return pl.pallas_call(
        finish_kernel,
        out_shape=(
            jax.ShapeDtypeStruct((1, 2, CH, 2, SIDE), F32),
            jax.ShapeDtypeStruct((9, width, C), F32),
        ),
        in_specs=[vmem] * 3,
        out_specs=(vmem, vmem),
        name="finish",
    )(own, other, w_out_t)


def local(noise, target, timesteps, w_in, gn_gain, w_time1, w_time2, w_conv, w_out):
    count = lax.axis_size("tensor")
    recv = lax.all_to_all(pack(noise, target), "tensor", 0, 0, tiled=True)
    w_out_t = w_out.T
    made = prepare(timesteps, w_out_t, w_in, gn_gain, w_time1, w_time2.T, w_conv)
    own = chain(timesteps, jnp.asarray(schedule_tables()), recv, *made, w_in)
    other = lax.ppermute(own, "tensor", [(i, i ^ 1) for i in range(count)])
    path, grad = finish(own, other, w_out_t, C // count)
    return path, jnp.swapaxes(grad, 1, 2)


def solution(mesh):
    placed = (
        P(None, None, "tensor", None),
        P(None, None, "tensor", None),
        P(),
        P(),
        P(),
        P(),
        P(),
        P(),
        P(),
    )
    return jax.shard_map(
        local,
        mesh=mesh,
        in_specs=placed,
        out_specs=(P("section", None, None, "tensor", None), P(None, None, "tensor")),
        check_vma=False,
    )
```

```python
import math

import jax
import jax.numpy as jnp
import numpy as np
from jax import lax
from jax.experimental import pallas as pl
from jax.experimental.pallas import tpu as pltpu
from jax.sharding import PartitionSpec as P


GROUPS = 32
STEPS = 16
CH = 4
C = 320
SIDE = 32
PIX = SIDE * SIDE
TILE = 256
F32 = jnp.float32
BF16 = jnp.bfloat16
EPS = 1e-05


def schedule_tables():
    grid = np.arange(1000, dtype=np.float64)
    low, high = math.sqrt(0.00085), math.sqrt(0.012)
    bar = np.cumprod(1.0 - (low + grid * ((high - low) / 999.0)) ** 2)
    table = np.zeros((3, 1024), np.float32)
    table[0, :1000] = np.sqrt(bar)
    table[1, :1000] = 1.0 / np.sqrt(bar)
    table[2, :1000] = np.sqrt(1.0 - bar)
    return table


def split(x, parts):
    out = []
    for _ in range(parts):
        head = x.astype(BF16)
        out.append(head)
        x = x - head.astype(F32)
    return out


def dot(a, b, dims=((1,), (0,)), precision=None):
    return lax.dot_general(a, b, (dims, ((), ())), precision=precision, preferred_element_type=F32)


NT = ((1,), (1,))


def rolled(x, shift, axis):
    return pltpu.roll(x, shift % x.shape[axis], axis)


def doubled(x):
    return jnp.concatenate([x, x], axis=0)


def row_index(shape):
    return lax.broadcasted_iota(jnp.int32, shape, 0)


def position():
    return lax.axis_index("section"), lax.axis_index("tensor")


def wave_tables():
    half = C // 2
    f = np.exp(-math.log(10000.0) * np.arange(half, dtype=np.float64) / half)
    step = np.arange(32, dtype=np.float64)[:, None]
    big, small = 32.0 * step * f, step * f
    both = lambda a, b: np.concatenate([a, b], axis=1)
    return np.stack(
        [
            both(np.cos(big), np.sin(big)),
            both(-np.sin(big), np.cos(big)),
            both(np.cos(small), np.cos(small)),
            both(np.sin(small), np.sin(small)),
        ]
    ).astype(np.float32)


def near(x):
    return pltpu.with_memory_space_constraint(x, pltpu.VMEM)


def pack_kernel(noise, target, packed):
    for m in range(2):
        parts = [x[m, :, r, :] for x in (noise, target) for r in range(2)]
        tile = jnp.concatenate(parts, axis=1)
        for j in range(8):
            packed[2 * j + m] = tile


def pack(noise, target):
    vmem = pl.BlockSpec(memory_space=pltpu.VMEM)
    return pl.pallas_call(
        pack_kernel,
        out_shape=pltpu.VMEM((16, CH, 128), F32),
        in_specs=[vmem] * 2,
        out_specs=vmem,
        name="pack",
    )(noise, target)


def regrouped(x, buffer):
    buffer[...] = x
    size = C // GROUPS
    return jnp.concatenate([buffer[pl.ds(k, GROUPS, stride=size), :] for k in range(size)], axis=0)


def two(x):
    head = x.astype(BF16)
    return head, (x - head.astype(F32)).astype(BF16)


def stacked(a, b):
    return jnp.concatenate([a.astype(F32), b.astype(F32)], axis=0).astype(BF16)


def prepare_kernel(
    times, tables, waves, w_out_t, w_in, gain, w1_hbm, w2t_hbm, conv_hbm,
    w_fwd, w_bwd, emb, rows, cols, spread, means, steps, w1, w2t, conv, buffer, sems,
):
    copies = [pltpu.make_async_copy(conv_hbm.at[k], conv.at[k], sems.at[k]) for k in range(9)]
    copies.append(pltpu.make_async_copy(w1_hbm, w1, sems.at[9]))
    copies.append(pltpu.make_async_copy(w2t_hbm, w2t, sems.at[10]))
    for c in copies:
        c.start()
    for s in range(STEPS):
        now = times[s]
        last = s == STEPS - 1
        root = 1.0 if last else tables[0, times[s + 1]]
        rest = 0.0 if last else tables[2, times[s + 1]]
        keep = root * tables[1, now]
        steps[0, s] = keep
        steps[1, s] = rest - keep * tables[2, now]
    out8 = doubled(w_out_t[...])
    in8 = doubled(w_in[...])
    first = row_index((8, C)) < CH
    next1, next2 = rolled(in8, -1, 0), rolled(in8, -2, 0)
    top = jnp.where(first, in8, in8 * in8)
    low = in8 * jnp.where(first, 2.0 * next1, next2)
    group = lambda axis: lax.broadcasted_iota(jnp.int32, (C, C), axis) * 6554 >> 16
    member = jnp.where(group(0) == group(1), 1.0, 0.0).astype(BF16)
    both = jnp.concatenate([top, low], axis=0)
    p1, p2, p3 = [p.astype(F32) for p in split(both, 3)]
    sums = dot(jnp.concatenate([p1, p2, p3], axis=0).astype(BF16), member)
    sums = (sums[0:16] + sums[16:32] + sums[32:48]) * (1.0 / (PIX * (C // GROUPS)))
    half_gain = 0.5 * gain[...].reshape(1, C)
    place8 = row_index((8, C))
    folded = jnp.where(place8 < CH, in8, jnp.where(place8 == CH, 1.0, 0.0)) * half_gain
    gain8 = jnp.broadcast_to(half_gain, (8, C))
    table = jnp.concatenate(
        [folded, folded, folded, in8, sums, gain8, jnp.zeros((72, C), F32)], axis=0
    )
    ordered = regrouped(table.T, buffer)
    spread[...] = ordered
    for j in range(16):
        means[j] = jnp.broadcast_to(ordered[0:GROUPS, 32 + j : 33 + j], (GROUPS, 128))
    turned = ordered.T
    for c in range(CH):
        rows[16 * (c + 1) : 16 * (c + 2)] = turned[32:48] * turned[24 + c : 25 + c]
    rows[0:16] = turned[32:48]
    rows[80:88] = turned[48:56]
    rows[88:96] = turned[24:32]
    for j in range(CH):
        ahead = jnp.sum(out8 * rolled(in8, -j, 0), axis=1, keepdims=True)
        back = jnp.sum(rolled(out8, -j, 0) * in8, axis=1, keepdims=True)
        cols[j] = jnp.broadcast_to(ahead, (8, 128))
        cols[CH + j] = jnp.broadcast_to(back, (8, 128))
    repeated = jnp.concatenate([out8] * 16, axis=0).T
    lane = lax.broadcasted_iota(jnp.int32, (C, 128), 1)
    r_head, r_tail = two(repeated)
    r_head, r_tail = r_head.astype(F32), r_tail.astype(F32)
    acc = jnp.zeros((C, 256), F32)
    for k in range(9):
        copies[k].wait()
    for k in range(9):
        at = lane // 8 == k
        right = jnp.concatenate([jnp.where(at, r_head, 0.0), jnp.where(at, r_tail, 0.0)], axis=1)
        acc = acc + dot(conv[k], right.astype(BF16))
    full = regrouped(acc[:, :128] + acc[:, 128:], buffer)
    head = full.astype(BF16).astype(F32)
    tail = full - head
    w_bwd[...] = jnp.concatenate([head[:, :80], tail[:, :80]], axis=1).astype(BF16)
    w_fwd[...] = jnp.where(lane % 8 < CH, head, tail).T[:80].astype(BF16)
    feats = []
    for s in range(STEPS):
        t = times[s]
        a, b = t >> 5, t & 31
        feats.append(
            waves[0, pl.ds(a, 1)] * waves[2, pl.ds(b, 1)]
            + waves[1, pl.ds(a, 1)] * waves[3, pl.ds(b, 1)]
        )
    f_head, f_tail = two(jnp.concatenate(feats, axis=0))
    o_head, o_tail = two(out8)
    copies[9].wait()
    w_head, w_tail = two(w1[...])
    z = dot(stacked(f_head, f_tail), w_head)
    z = 0.5 * (z[:STEPS] + z[STEPS:] + dot(f_head, w_tail))
    hidden = z + z * jnp.tanh(z)
    copies[10].wait()
    w_head, w_tail = two(w2t[...])
    y = dot(stacked(o_head, o_tail), w_head)
    y = y[0:8] + y[8:16] + dot(o_head, w_tail)
    y_head, y_tail = two(y)
    h_head, h_tail = two(hidden)
    x = dot(stacked(y_head, y_tail), h_head, NT)
    shift = x[0:8] + x[8:16] + dot(y_head, h_tail, NT)
    for s in range(STEPS):
        emb[s] = jnp.broadcast_to(shift[:, s : s + 1], (8, 128))


def prepare(times, w_out_t, w_in, gain, w1, w2t, w_conv):
    smem = pl.BlockSpec(memory_space=pltpu.SMEM)
    vmem = pl.BlockSpec(memory_space=pltpu.VMEM)
    hbm = pl.BlockSpec(memory_space=pl.ANY)
    return pl.pallas_call(
        prepare_kernel,
        out_shape=(
            pltpu.VMEM((80, C), BF16),
            pltpu.VMEM((C, 160), BF16),
            pltpu.VMEM((STEPS, 8, 128), F32),
            pltpu.VMEM((96, C), F32),
            pltpu.VMEM((8, 8, 128), F32),
            pltpu.VMEM((C, 128), F32),
            pltpu.VMEM((16, GROUPS, 128), F32),
            pltpu.SMEM((2, STEPS), F32),
        ),
        in_specs=[smem] * 2 + [vmem] * 4 + [hbm] * 3,
        out_specs=(vmem,) * 7 + (smem,),
        scratch_shapes=[
            pltpu.VMEM(w1.shape, F32),
            pltpu.VMEM(w2t.shape, F32),
            pltpu.VMEM(w_conv.shape, BF16),
            pltpu.VMEM((C, 128), F32),
            pltpu.SemaphoreType.DMA((11,)),
        ],
        name="prepare",
    )(times, jnp.asarray(schedule_tables()), jnp.asarray(wave_tables()), w_out_t, w_in, gain, w1, w2t, w_conv)


def wide(col):
    return jnp.concatenate([col] * (PIX // 128), axis=1)


def chain_kernel(
    recv, w_fwd, w_bwd, emb, rows, cols, spread, means, steps,
    sent, lat, stat, act, half, slope, taps, total, ordered,
):
    section, index = position()
    rid = row_index((8, PIX))
    upper = rid < CH
    lane = lax.broadcasted_iota(jnp.int32, (8, 128), 1)
    column = lane % SIDE
    col_ok = {1: column > 0, 0: None, -1: column < SIDE - 1}
    low_ok, high_ok = lane >= SIDE, lane < 128 - SIDE
    supper = row_index((8, C)) < CH
    glane = lax.broadcasted_iota(jnp.int32, (GROUPS, 128), 1)
    slane = lax.broadcasted_iota(jnp.int32, (C, 128), 1)
    in8 = rows[88:96]
    half_gain = rows[80:81]

    def piece(x, v):
        return x[:, 128 * v : 128 * v + 128]

    def moved(x, d):
        return x if d == 0 else jnp.where(col_ok[d], rolled(x, d, 1), 0.0)

    def moved_low(x, d):
        y = rolled(x, SIDE + d, 1)
        return jnp.where(low_ok if d == 0 else low_ok & col_ok[d], y, 0.0)

    def moved_high(x, d):
        y = rolled(x, d - SIDE, 1)
        return jnp.where(high_ok if d == 0 else high_ok & col_ok[d], y, 0.0)

    got = [recv[i] for i in range(16)]

    def gathered(base):
        parts = []
        for v in range(8):
            at = base + SIDE * (v % 2)
            parts.extend(got[(8 * q + v) // 2][:, at : at + SIDE] for q in range(4))
        return doubled(jnp.concatenate(parts, axis=1))

    latent0, target8 = gathered(0), gathered(2 * SIDE)

    def coefs(s):
        return steps[0, s], steps[1, s]

    def forward(s, l8):
        keep, nc = coefs(s)
        lat[s] = l8
        r1, r2, r3 = rolled(l8, -1, 0), rolled(l8, -2, 0), rolled(l8, -3, 0)
        x0 = jnp.where(upper, l8, l8 * l8)
        x1 = l8 * jnp.where(upper, r1, r2)
        m0 = jnp.sum(x0, axis=1, keepdims=True)
        m1 = jnp.sum(x1, axis=1, keepdims=True)
        p0 = rows[0:8] * m0
        p1 = rows[8:16] * m1
        avg = jnp.sum(jnp.where(supper, p0, 0.0), axis=0, keepdims=True)
        sq = jnp.sum(jnp.where(supper, 0.0, p0) + p1, axis=0, keepdims=True)
        rstd = lax.rsqrt(sq - avg * avg + EPS)
        scale = rstd * half_gain
        stat[s, 0:1] = avg
        stat[s, 1:2] = rstd
        stat[s, 2:3] = scale
        k0, k1 = jnp.broadcast_to(m0, (8, 128)), jnp.broadcast_to(m1, (8, 128))
        terms = [means[j] * k0[j : j + 1] for j in range(8)]
        terms += [means[8 + j] * k1[j : j + 1] for j in range(8)]
        gavg = (terms[0] + terms[1]) + (terms[2] + terms[3])
        gsq = ((terms[4] + terms[5]) + (terms[6] + terms[7])) + (
            ((terms[8] + terms[9]) + (terms[10] + terms[11]))
            + ((terms[12] + terms[13]) + (terms[14] + terms[15]))
        )
        factor = lax.rsqrt(gsq - gavg * gavg + EPS)
        factor = jnp.where(glane % 8 == CH, -gavg * factor, factor)
        wz = spread[...] * jnp.concatenate([factor] * (C // GROUPS), axis=0)
        a = wz.astype(BF16).astype(F32)
        wzs = jnp.where(slane >= 16, wz - a, a).astype(BF16)[:, :24]
        hom = jnp.where(upper, l8, jnp.where(rid == CH, 1.0, 0.0))
        d = hom.astype(BF16).astype(F32)
        ls = jnp.concatenate([d, hom - d, d], axis=0).astype(BF16)
        linear = (
            wide(cols[0]) * l8 + wide(cols[1]) * r1 + wide(cols[2]) * r2 + wide(cols[3]) * r3
        )
        linear = keep * l8 + nc * (linear + wide(emb[s]))
        tiles = [slice(j * TILE, (j + 1) * TILE) for j in range(PIX // TILE)]
        hs = [dot(wzs, ls[:, at]) for at in tiles]
        for at, h in zip(tiles, hs):
            t = jnp.tanh(h)
            u = h * t
            narrow = (h + u).astype(BF16)
            act[s, :, at] = narrow
            taps[:, at] = dot(w_fwd[...], narrow)
            half[s, :, at] = t.astype(BF16)

        def tap(dy, dx, v):
            k = 8 * (3 * dy + dx)
            return taps[k : k + 8, 128 * v : 128 * v + 128]

        out = []
        for v in range(8):
            conv = None
            for dx in (1, 0, 2):
                d = 1 - dx
                part = tap(1, dx, v)
                if v > 0:
                    part = part + tap(0, dx, v - 1)
                if v < 7:
                    part = part + tap(2, dx, v + 1)
                part = moved(part, d)
                conv = part if conv is None else conv + part
                if v == 0:
                    conv = conv + moved_low(tap(0, dx, 7), d)
                if v == 7:
                    conv = conv + moved_high(tap(2, dx, 0), d)
            conv = conv + rolled(conv, 4, 0)
            out.append(piece(linear, v) + nc * conv)
        return jnp.concatenate(out, axis=1)

    final = lax.fori_loop(0, STEPS, forward, latent0)
    lat[STEPS] = final
    total[...] = jnp.zeros_like(total)
    erow = row_index((16, C)) < CH

    def backward(i, adj):
        s = STEPS - 1 - i
        keep, nc = coefs(s)
        l8 = lat[s]
        avg, rstd, scale = stat[s, 0:1], stat[s, 1:2], stat[s, 2:3]
        ng = nc * adj
        head = ng.astype(BF16).astype(F32)
        x = jnp.where(upper, head, ng - head)
        first, last = piece(x, 0), piece(x, 7)
        above, same, below = [], [], []
        for d in (-1, 0, 1):
            ys = [moved(piece(x, v), d) for v in range(8)]
            same.append(jnp.concatenate(ys, axis=1))
            above.append(jnp.concatenate(ys[1:] + [moved_high(first, d)], axis=1))
            below.append(jnp.concatenate([moved_low(last, d)] + ys[:7], axis=1))
        pad = jnp.zeros_like(x)
        a80 = jnp.concatenate(above + same + below + [pad], axis=0).astype(BF16)
        col = jnp.concatenate([a80, a80], axis=0)
        ws = in8 * scale
        whead = ws.astype(BF16).astype(F32)
        wd = jnp.where(supper, whead, ws - whead)
        q = (-0.5 * rstd * rstd * rstd) * half_gain
        qa = q * avg
        per = jnp.where(erow, -2.0 * qa, q)
        one = jnp.where(erow, 2.0 * qa * avg - scale, -qa)
        phi = [rows[16 * (c + 1) : 16 * (c + 2)] * per for c in range(CH)]
        phi = jnp.concatenate(phi + [rows[0:16] * one, wd, jnp.zeros_like(wd)], axis=0).astype(BF16)
        tiles = [slice(j * TILE, (j + 1) * TILE) for j in range(PIX // TILE)]
        for at in tiles:
            t = half[s, :, at]
            slope[:, at] = (1 + t) + act[s, :, at] * (1 - t)
        gs = [dot(w_bwd[...], col[:, at]) for at in tiles]
        mid = PIX // 2
        total[...] += dot(act[s, :, :mid], a80[:, :mid], NT)
        outs = []
        for at, g in zip(tiles, gs):
            outs.append(dot(phi, g.astype(BF16) * slope[:, at]))
        total[...] += dot(act[s, :, mid:], a80[:, mid:], NT)
        z = jnp.concatenate(outs, axis=1)
        dl = z[80:88]
        dl = dl + rolled(dl, 4, 0)
        acc0, acc1 = z[64:72], z[72:80]
        for c in range(CH):
            lc = l8[c : c + 1]
            acc0 = acc0 + z[16 * c : 16 * c + 8] * lc
            acc1 = acc1 + z[16 * c + 8 : 16 * c + 16] * lc
        c0 = jnp.sum(acc0, axis=1, keepdims=True)
        c1 = jnp.sum(acc1, axis=1, keepdims=True)
        c0 = jnp.broadcast_to(c0, (8, 128))
        c1 = jnp.broadcast_to(c1, (8, 128))
        up8 = upper[:, :128]
        c0r, c1r = rolled(c0, 4, 0), rolled(c1, 4, 0)
        dm = jnp.where(up8, c0, c0r)
        d0 = 2.0 * jnp.where(up8, c0r, c0)
        d1 = jnp.where(up8, c1, c1r)
        d3 = rolled(d1, 1, 0)
        d2 = jnp.where(up8, c1r, c1)
        d2 = d2 + rolled(d2, 2, 0)
        r1, r2, r3 = rolled(l8, -1, 0), rolled(l8, -2, 0), rolled(l8, -3, 0)
        a1, a2, a3 = rolled(adj, -1, 0), rolled(adj, -2, 0), rolled(adj, -3, 0)
        linear = (
            wide(cols[4]) * adj + wide(cols[5]) * a1 + wide(cols[6]) * a2 + wide(cols[7]) * a3
        )
        linear = keep * adj + nc * linear + dl
        stats = wide(dm) + wide(d0) * l8 + wide(d1) * r1 + wide(d2) * r2 + wide(d3) * r3
        return linear + stats

    lax.fori_loop(0, STEPS, backward, final - target8)
    size = C // GROUPS
    for k in range(size):
        ordered[pl.ds(k, GROUPS, stride=size), 0:80] = total[GROUPS * k : GROUPS * k + GROUPS]
    turned = ordered[:, 0:80].T
    for k in range(9):
        part = turned[8 * k : 8 * k + 8]
        part = part + rolled(part, 4, 0)
        sent[4 * k : 4 * k + 4] = part[0:4]
    mine = lat[section + 1, :, pl.ds(pl.multiple_of(index % 4 // 2 * 512, 512), 512)]
    blank = jnp.zeros((4, C - 128), F32)
    for v in range(4):
        sent[36 + 4 * v : 40 + 4 * v] = jnp.concatenate([piece(mine, v)[0:4], blank], axis=1)


def chain(recv, w_fwd, w_bwd, emb, rows, cols, spread, means, steps):
    smem = pl.BlockSpec(memory_space=pltpu.SMEM)
    vmem = pl.BlockSpec(memory_space=pltpu.VMEM)
    return pl.pallas_call(
        chain_kernel,
        out_shape=pltpu.VMEM((56, C), F32),
        in_specs=[vmem] * 8 + [smem],
        out_specs=vmem,
        scratch_shapes=[
            pltpu.VMEM((STEPS + 1, 8, PIX), F32),
            pltpu.VMEM((STEPS, 8, C), F32),
            pltpu.VMEM((STEPS, C, PIX), BF16),
            pltpu.VMEM((STEPS, C, PIX), BF16),
            pltpu.VMEM((C, PIX), BF16),
            pltpu.VMEM((80, PIX), F32),
            pltpu.VMEM((C, 80), F32),
            pltpu.VMEM((C, 128), F32),
        ],
        name="chain",
    )(*[near(x) for x in (recv, w_fwd, w_bwd, emb, rows, cols, spread, means)], steps)


def finish_kernel(own, other, w_out_t, path, grad):
    index = position()[1]
    core, turn = index % 2, (128 - SIDE * (index // 4)) % 128
    for r in range(2):
        k = 36 + 4 * r
        mine = jnp.where(core == 0, own[k : k + 4, 0:128], own[k + 8 : k + 12, 0:128])
        theirs = jnp.where(core == 0, other[k : k + 4, 0:128], other[k + 8 : k + 12, 0:128])
        first = jnp.where(core == 0, mine, theirs)
        second = jnp.where(core == 0, theirs, mine)
        for m, x in enumerate((first, second)):
            x = pltpu.roll(x, turn, 1)
            for c in range(CH):
                path[0, m, c, r : r + 1] = x[c : c + 1, 0:SIDE]
    width = grad.shape[1]
    weights = jnp.concatenate([w_out_t[...], jnp.zeros((CH, 384 - C), F32)], axis=1)
    weights = pltpu.roll(weights, (384 - width * index) % 384, 1)[:, :128]
    w_head = weights.astype(BF16).astype(F32)
    left = jnp.concatenate([w_head, w_head, weights - w_head, weights * 0.0], axis=0)
    left = left.T[:24].astype(BF16)
    both = own[0:36] + other[0:36]
    head = both.astype(BF16).astype(F32)
    tail = both - head
    for k in range(9):
        at = slice(4 * k, 4 * k + 4)
        right = jnp.concatenate([head[at], tail[at], head[at], tail[at]], axis=0)
        grad[k] = dot(left, right.astype(BF16))[:width]


def finish(own, other, w_out_t, width):
    vmem = pl.BlockSpec(memory_space=pltpu.VMEM)
    return pl.pallas_call(
        finish_kernel,
        out_shape=(
            jax.ShapeDtypeStruct((1, 2, CH, 2, SIDE), F32),
            jax.ShapeDtypeStruct((9, width, C), F32),
        ),
        in_specs=[vmem] * 3,
        out_specs=(vmem, vmem),
        name="finish",
    )(own, other, w_out_t)


def local(noise, target, timesteps, w_in, gn_gain, w_time1, w_time2, w_conv, w_out):
    count = lax.axis_size("tensor")
    recv = lax.all_to_all(pack(noise, target), "tensor", 0, 0, tiled=True)
    w_out_t = w_out.T
    made = prepare(timesteps, w_out_t, w_in, gn_gain, w_time1, w_time2.T, w_conv)
    own = chain(recv, *made)
    other = lax.ppermute(own, "tensor", [(i, i ^ 1) for i in range(count)])
    path, grad = finish(near(own), near(other), near(w_out_t), C // count)
    return path, jnp.swapaxes(grad, 1, 2)


def solution(mesh):
    placed = (
        P(None, None, "tensor", None),
        P(None, None, "tensor", None),
        P(),
        P(),
        P(),
        P(),
        P(),
        P(),
        P(),
    )
    return jax.shard_map(
        local,
        mesh=mesh,
        in_specs=placed,
        out_specs=(P("section", None, None, "tensor", None), P(None, None, "tensor")),
        check_vma=False,
    )
```

```python
import math

import jax
import jax.numpy as jnp
import numpy as np
from jax import lax
from jax.experimental import pallas as pl
from jax.experimental.pallas import tpu as pltpu
from jax.sharding import PartitionSpec as P


GROUPS = 32
STEPS = 16
CH = 4
C = 320
SIDE = 32
PIX = SIDE * SIDE
TILE = 256
F32 = jnp.float32
BF16 = jnp.bfloat16
EPS = 1e-05


def schedule_tables():
    grid = np.arange(1000, dtype=np.float64)
    low, high = math.sqrt(0.00085), math.sqrt(0.012)
    bar = np.cumprod(1.0 - (low + grid * ((high - low) / 999.0)) ** 2)
    table = np.zeros((3, 1024), np.float32)
    table[0, :1000] = np.sqrt(bar)
    table[1, :1000] = 1.0 / np.sqrt(bar)
    table[2, :1000] = np.sqrt(1.0 - bar)
    return table


def split(x, parts):
    out = []
    for _ in range(parts):
        head = x.astype(BF16)
        out.append(head)
        x = x - head.astype(F32)
    return out


def dot(a, b, dims=((1,), (0,)), precision=None):
    return lax.dot_general(a, b, (dims, ((), ())), precision=precision, preferred_element_type=F32)


NT = ((1,), (1,))


def rolled(x, shift, axis):
    return pltpu.roll(x, shift % x.shape[axis], axis)


def doubled(x):
    return jnp.concatenate([x, x], axis=0)


def row_index(shape):
    return lax.broadcasted_iota(jnp.int32, shape, 0)


def position():
    return lax.axis_index("section"), lax.axis_index("tensor")


def wave_tables():
    half = C // 2
    f = np.exp(-math.log(10000.0) * np.arange(half, dtype=np.float64) / half)
    step = np.arange(32, dtype=np.float64)[:, None]
    big, small = 32.0 * step * f, step * f
    both = lambda a, b: np.concatenate([a, b], axis=1)
    return np.stack(
        [
            both(np.cos(big), np.sin(big)),
            both(-np.sin(big), np.cos(big)),
            both(np.cos(small), np.cos(small)),
            both(np.sin(small), np.sin(small)),
        ]
    ).astype(np.float32)


def near(x):
    return pltpu.with_memory_space_constraint(x, pltpu.VMEM)


def pack_kernel(noise, target, packed):
    for m in range(2):
        parts = [x[m, :, r, :] for x in (noise, target) for r in range(2)]
        tile = jnp.concatenate(parts, axis=1)
        for j in range(8):
            packed[2 * j + m] = tile


def pack(noise, target):
    vmem = pl.BlockSpec(memory_space=pltpu.VMEM)
    return pl.pallas_call(
        pack_kernel,
        out_shape=pltpu.VMEM((16, CH, 128), F32),
        in_specs=[vmem] * 2,
        out_specs=vmem,
        name="pack",
    )(noise, target)


def regrouped(x, buffer):
    buffer[...] = x
    size = C // GROUPS
    return jnp.concatenate([buffer[pl.ds(k, GROUPS, stride=size), :] for k in range(size)], axis=0)


def two(x):
    head = x.astype(BF16)
    return head, (x - head.astype(F32)).astype(BF16)


def stacked(a, b):
    return jnp.concatenate([a.astype(F32), b.astype(F32)], axis=0).astype(BF16)


def prepare_kernel(
    times, tables, waves, w_out_t, w_in, gain, w1_hbm, w2t_hbm, conv_hbm,
    w_fwd, w_bwd, emb, rows, cols, spread, means, steps, w1, w2t, conv, buffer, sems,
):
    copies = [pltpu.make_async_copy(conv_hbm.at[k], conv.at[k], sems.at[k]) for k in range(9)]
    copies.append(pltpu.make_async_copy(w1_hbm, w1, sems.at[9]))
    copies.append(pltpu.make_async_copy(w2t_hbm, w2t, sems.at[10]))
    for c in copies:
        c.start()
    for s in range(STEPS):
        now = times[s]
        last = s == STEPS - 1
        root = 1.0 if last else tables[0, times[s + 1]]
        rest = 0.0 if last else tables[2, times[s + 1]]
        keep = root * tables[1, now]
        steps[0, s] = keep
        steps[1, s] = rest - keep * tables[2, now]
    out8 = doubled(w_out_t[...])
    in8 = doubled(w_in[...])
    first = row_index((8, C)) < CH
    next1, next2 = rolled(in8, -1, 0), rolled(in8, -2, 0)
    top = jnp.where(first, in8, in8 * in8)
    low = in8 * jnp.where(first, 2.0 * next1, next2)
    group = lambda axis: lax.broadcasted_iota(jnp.int32, (C, C), axis) * 6554 >> 16
    member = jnp.where(group(0) == group(1), 1.0, 0.0).astype(BF16)
    both = jnp.concatenate([top, low], axis=0)
    p1, p2, p3 = [p.astype(F32) for p in split(both, 3)]
    sums = dot(jnp.concatenate([p1, p2, p3], axis=0).astype(BF16), member)
    sums = (sums[0:16] + sums[16:32] + sums[32:48]) * (1.0 / (PIX * (C // GROUPS)))
    half_gain = 0.5 * gain[...].reshape(1, C)
    place8 = row_index((8, C))
    folded = jnp.where(place8 < CH, in8, jnp.where(place8 == CH, 1.0, 0.0)) * half_gain
    gain8 = jnp.broadcast_to(half_gain, (8, C))
    table = jnp.concatenate(
        [folded, folded, folded, in8, sums, gain8, jnp.zeros((72, C), F32)], axis=0
    )
    ordered = regrouped(table.T, buffer)
    spread[...] = ordered
    for j in range(16):
        means[j] = jnp.broadcast_to(ordered[0:GROUPS, 32 + j : 33 + j], (GROUPS, 128))
    turned = ordered.T
    for c in range(CH):
        rows[16 * (c + 1) : 16 * (c + 2)] = turned[32:48] * turned[24 + c : 25 + c]
    rows[0:16] = turned[32:48]
    rows[80:88] = turned[48:56]
    rows[88:96] = turned[24:32]
    for j in range(CH):
        ahead = jnp.sum(out8 * rolled(in8, -j, 0), axis=1, keepdims=True)
        back = jnp.sum(rolled(out8, -j, 0) * in8, axis=1, keepdims=True)
        cols[j] = jnp.broadcast_to(ahead, (8, 128))
        cols[CH + j] = jnp.broadcast_to(back, (8, 128))
    repeated = jnp.concatenate([out8] * 16, axis=0).T
    lane = lax.broadcasted_iota(jnp.int32, (C, 128), 1)
    r_head, r_tail = two(repeated)
    r_head, r_tail = r_head.astype(F32), r_tail.astype(F32)
    acc = jnp.zeros((C, 256), F32)
    for k in range(9):
        copies[k].wait()
    for k in range(9):
        at = lane // 8 == k
        right = jnp.concatenate([jnp.where(at, r_head, 0.0), jnp.where(at, r_tail, 0.0)], axis=1)
        acc = acc + dot(conv[k], right.astype(BF16))
    full = regrouped(acc[:, :128] + acc[:, 128:], buffer)
    head = full.astype(BF16).astype(F32)
    tail = full - head
    w_bwd[...] = jnp.concatenate([head[:, :80], tail[:, :80]], axis=1).astype(BF16)
    w_fwd[...] = jnp.where(lane % 8 < CH, head, tail).T[:80].astype(BF16)
    feats = []
    for s in range(STEPS):
        t = times[s]
        a, b = t >> 5, t & 31
        feats.append(
            waves[0, pl.ds(a, 1)] * waves[2, pl.ds(b, 1)]
            + waves[1, pl.ds(a, 1)] * waves[3, pl.ds(b, 1)]
        )
    f_head, f_tail = two(jnp.concatenate(feats, axis=0))
    o_head, o_tail = two(out8)
    copies[9].wait()
    copies[10].wait()
    w_head, w_tail = two(w1[...])
    z = dot(stacked(f_head, f_tail), w_head)
    z = 0.5 * (z[:STEPS] + z[STEPS:] + dot(f_head, w_tail))
    hidden = z + z * jnp.tanh(z)
    w_head, w_tail = two(w2t[...])
    y = dot(stacked(o_head, o_tail), w_head)
    y = y[0:8] + y[8:16] + dot(o_head, w_tail)
    y_head, y_tail = two(y)
    h_head, h_tail = two(hidden)
    x = dot(stacked(y_head, y_tail), h_head, NT)
    shift = x[0:8] + x[8:16] + dot(y_head, h_tail, NT)
    for s in range(STEPS):
        emb[s] = jnp.broadcast_to(shift[:, s : s + 1], (8, 128))


def prepare(times, w_out_t, w_in, gain, w1, w2t, w_conv):
    smem = pl.BlockSpec(memory_space=pltpu.SMEM)
    vmem = pl.BlockSpec(memory_space=pltpu.VMEM)
    hbm = pl.BlockSpec(memory_space=pl.ANY)
    return pl.pallas_call(
        prepare_kernel,
        out_shape=(
            pltpu.VMEM((80, C), BF16),
            pltpu.VMEM((C, 160), BF16),
            pltpu.VMEM((STEPS, 8, 128), F32),
            pltpu.VMEM((96, C), F32),
            pltpu.VMEM((8, 8, 128), F32),
            pltpu.VMEM((C, 128), F32),
            pltpu.VMEM((16, GROUPS, 128), F32),
            pltpu.SMEM((2, STEPS), F32),
        ),
        in_specs=[smem] * 2 + [vmem] * 4 + [hbm] * 3,
        out_specs=(vmem,) * 7 + (smem,),
        scratch_shapes=[
            pltpu.VMEM(w1.shape, F32),
            pltpu.VMEM(w2t.shape, F32),
            pltpu.VMEM(w_conv.shape, BF16),
            pltpu.VMEM((C, 128), F32),
            pltpu.SemaphoreType.DMA((11,)),
        ],
        name="prepare",
    )(times, jnp.asarray(schedule_tables()), jnp.asarray(wave_tables()), w_out_t, w_in, gain, w1, w2t, w_conv)


def repeated(step, state, group):
    def several(i, state):
        for k in range(group):
            state = step(group * i + k, state)
        return state

    return lax.fori_loop(0, STEPS // group, several, state)


def wide(col):
    return jnp.concatenate([col] * (PIX // 128), axis=1)


def chain_kernel(
    recv, w_fwd, w_bwd, emb, rows, cols, spread, means, steps,
    sent, lat, stat, act, half, slope, taps, total, ordered,
):
    section, index = position()
    rid = row_index((8, PIX))
    upper = rid < CH
    lane = lax.broadcasted_iota(jnp.int32, (8, 128), 1)
    column = lane % SIDE
    col_ok = {1: column > 0, 0: None, -1: column < SIDE - 1}
    low_ok, high_ok = lane >= SIDE, lane < 128 - SIDE
    supper = row_index((8, C)) < CH
    glane = lax.broadcasted_iota(jnp.int32, (GROUPS, 128), 1)
    slane = lax.broadcasted_iota(jnp.int32, (C, 128), 1)
    in8 = rows[88:96]
    half_gain = rows[80:81]

    def piece(x, v):
        return x[:, 128 * v : 128 * v + 128]

    def moved(x, d):
        return x if d == 0 else jnp.where(col_ok[d], rolled(x, d, 1), 0.0)

    def moved_low(x, d):
        y = rolled(x, SIDE + d, 1)
        return jnp.where(low_ok if d == 0 else low_ok & col_ok[d], y, 0.0)

    def moved_high(x, d):
        y = rolled(x, d - SIDE, 1)
        return jnp.where(high_ok if d == 0 else high_ok & col_ok[d], y, 0.0)

    got = [recv[i] for i in range(16)]

    def gathered(base):
        parts = []
        for v in range(8):
            at = base + SIDE * (v % 2)
            parts.extend(got[(8 * q + v) // 2][:, at : at + SIDE] for q in range(4))
        return doubled(jnp.concatenate(parts, axis=1))

    latent0, target8 = gathered(0), gathered(2 * SIDE)

    def coefs(s):
        return steps[0, s], steps[1, s]

    def forward(s, l8):
        keep, nc = coefs(s)
        lat[s] = l8
        r1, r2, r3 = rolled(l8, -1, 0), rolled(l8, -2, 0), rolled(l8, -3, 0)
        x0 = jnp.where(upper, l8, l8 * l8)
        x1 = l8 * jnp.where(upper, r1, r2)
        m0 = jnp.sum(x0, axis=1, keepdims=True)
        m1 = jnp.sum(x1, axis=1, keepdims=True)
        p0 = rows[0:8] * m0
        p1 = rows[8:16] * m1
        avg = jnp.sum(jnp.where(supper, p0, 0.0), axis=0, keepdims=True)
        sq = jnp.sum(jnp.where(supper, 0.0, p0) + p1, axis=0, keepdims=True)
        rstd = lax.rsqrt(sq - avg * avg + EPS)
        scale = rstd * half_gain
        stat[s, 0:1] = avg
        stat[s, 1:2] = rstd
        stat[s, 2:3] = scale
        k0, k1 = jnp.broadcast_to(m0, (8, 128)), jnp.broadcast_to(m1, (8, 128))
        terms = [means[j] * k0[j : j + 1] for j in range(8)]
        terms += [means[8 + j] * k1[j : j + 1] for j in range(8)]
        gavg = (terms[0] + terms[1]) + (terms[2] + terms[3])
        gsq = ((terms[4] + terms[5]) + (terms[6] + terms[7])) + (
            ((terms[8] + terms[9]) + (terms[10] + terms[11]))
            + ((terms[12] + terms[13]) + (terms[14] + terms[15]))
        )
        factor = lax.rsqrt(gsq - gavg * gavg + EPS)
        factor = jnp.where(glane % 8 == CH, -gavg * factor, factor)
        wz = spread[...] * jnp.concatenate([factor] * (C // GROUPS), axis=0)
        a = wz.astype(BF16).astype(F32)
        wzs = jnp.where(slane >= 16, wz - a, a).astype(BF16)[:, :24]
        hom = jnp.where(upper, l8, jnp.where(rid == CH, 1.0, 0.0))
        d = hom.astype(BF16).astype(F32)
        ls = jnp.concatenate([d, hom - d, d], axis=0).astype(BF16)
        linear = (
            wide(cols[0]) * l8 + wide(cols[1]) * r1 + wide(cols[2]) * r2 + wide(cols[3]) * r3
        )
        linear = keep * l8 + nc * (linear + wide(emb[s]))
        tiles = [slice(j * TILE, (j + 1) * TILE) for j in range(PIX // TILE)]
        hs = [dot(wzs, ls[:, at]) for at in tiles]
        for at, h in zip(tiles, hs):
            t = jnp.tanh(h)
            u = h * t
            narrow = (h + u).astype(BF16)
            act[s, :, at] = narrow
            taps[:, at] = dot(w_fwd[...], narrow)
            half[s, :, at] = t.astype(BF16)

        def tap(dy, dx, v):
            k = 8 * (3 * dy + dx)
            return taps[k : k + 8, 128 * v : 128 * v + 128]

        out = []
        for v in range(8):
            conv = None
            for dx in (1, 0, 2):
                d = 1 - dx
                part = tap(1, dx, v)
                if v > 0:
                    part = part + tap(0, dx, v - 1)
                if v < 7:
                    part = part + tap(2, dx, v + 1)
                part = moved(part, d)
                conv = part if conv is None else conv + part
                if v == 0:
                    conv = conv + moved_low(tap(0, dx, 7), d)
                if v == 7:
                    conv = conv + moved_high(tap(2, dx, 0), d)
            conv = conv + rolled(conv, 4, 0)
            out.append(piece(linear, v) + nc * conv)
        return jnp.concatenate(out, axis=1)

    final = repeated(forward, latent0, 2)
    lat[STEPS] = final
    total[...] = jnp.zeros_like(total)
    erow = row_index((16, C)) < CH

    def backward(i, adj):
        s = STEPS - 1 - i
        keep, nc = coefs(s)
        l8 = lat[s]
        avg, rstd, scale = stat[s, 0:1], stat[s, 1:2], stat[s, 2:3]
        ng = nc * adj
        head = ng.astype(BF16).astype(F32)
        x = jnp.where(upper, head, ng - head)
        first, last = piece(x, 0), piece(x, 7)
        above, same, below = [], [], []
        for d in (-1, 0, 1):
            ys = [moved(piece(x, v), d) for v in range(8)]
            same.append(jnp.concatenate(ys, axis=1))
            above.append(jnp.concatenate(ys[1:] + [moved_high(first, d)], axis=1))
            below.append(jnp.concatenate([moved_low(last, d)] + ys[:7], axis=1))
        pad = jnp.zeros_like(x)
        a80 = jnp.concatenate(above + same + below + [pad], axis=0).astype(BF16)
        col = jnp.concatenate([a80, a80], axis=0)
        ws = in8 * scale
        whead = ws.astype(BF16).astype(F32)
        wd = jnp.where(supper, whead, ws - whead)
        q = (-0.5 * rstd * rstd * rstd) * half_gain
        qa = q * avg
        per = jnp.where(erow, -2.0 * qa, q)
        one = jnp.where(erow, 2.0 * qa * avg - scale, -qa)
        phi = [rows[16 * (c + 1) : 16 * (c + 2)] * per for c in range(CH)]
        phi = jnp.concatenate(phi + [rows[0:16] * one, wd, jnp.zeros_like(wd)], axis=0).astype(BF16)
        tiles = [slice(j * TILE, (j + 1) * TILE) for j in range(PIX // TILE)]
        for at in tiles:
            t = half[s, :, at]
            slope[:, at] = (1 + t) + act[s, :, at] * (1 - t)
        gs = [dot(w_bwd[...], col[:, at]) for at in tiles]
        outs = []
        for at, g in zip(tiles, gs):
            outs.append(dot(phi, g.astype(BF16) * slope[:, at]))
        total[...] += dot(act[s], a80, NT)
        z = jnp.concatenate(outs, axis=1)
        dl = z[80:88]
        dl = dl + rolled(dl, 4, 0)
        acc0, acc1 = z[64:72], z[72:80]
        for c in range(CH):
            lc = l8[c : c + 1]
            acc0 = acc0 + z[16 * c : 16 * c + 8] * lc
            acc1 = acc1 + z[16 * c + 8 : 16 * c + 16] * lc
        c0 = jnp.sum(acc0, axis=1, keepdims=True)
        c1 = jnp.sum(acc1, axis=1, keepdims=True)
        c0 = jnp.broadcast_to(c0, (8, 128))
        c1 = jnp.broadcast_to(c1, (8, 128))
        up8 = upper[:, :128]
        c0r, c1r = rolled(c0, 4, 0), rolled(c1, 4, 0)
        dm = jnp.where(up8, c0, c0r)
        d0 = 2.0 * jnp.where(up8, c0r, c0)
        d1 = jnp.where(up8, c1, c1r)
        d3 = rolled(d1, 1, 0)
        d2 = jnp.where(up8, c1r, c1)
        d2 = d2 + rolled(d2, 2, 0)
        r1, r2, r3 = rolled(l8, -1, 0), rolled(l8, -2, 0), rolled(l8, -3, 0)
        a1, a2, a3 = rolled(adj, -1, 0), rolled(adj, -2, 0), rolled(adj, -3, 0)
        linear = (
            wide(cols[4]) * adj + wide(cols[5]) * a1 + wide(cols[6]) * a2 + wide(cols[7]) * a3
        )
        linear = keep * adj + nc * linear + dl
        stats = wide(dm) + wide(d0) * l8 + wide(d1) * r1 + wide(d2) * r2 + wide(d3) * r3
        return linear + stats

    repeated(backward, final - target8, 4)
    size = C // GROUPS
    for k in range(size):
        ordered[pl.ds(k, GROUPS, stride=size), 0:80] = total[GROUPS * k : GROUPS * k + GROUPS]
    turned = ordered[:, 0:80].T
    for k in range(9):
        part = turned[8 * k : 8 * k + 8]
        part = part + rolled(part, 4, 0)
        sent[4 * k : 4 * k + 4] = part[0:4]
    mine = lat[section + 1, :, pl.ds(pl.multiple_of(index % 4 // 2 * 512, 512), 512)]
    blank = jnp.zeros((4, C - 128), F32)
    for v in range(4):
        sent[36 + 4 * v : 40 + 4 * v] = jnp.concatenate([piece(mine, v)[0:4], blank], axis=1)


def chain(recv, w_fwd, w_bwd, emb, rows, cols, spread, means, steps):
    smem = pl.BlockSpec(memory_space=pltpu.SMEM)
    vmem = pl.BlockSpec(memory_space=pltpu.VMEM)
    return pl.pallas_call(
        chain_kernel,
        out_shape=pltpu.VMEM((56, C), F32),
        in_specs=[vmem] * 8 + [smem],
        out_specs=vmem,
        scratch_shapes=[
            pltpu.VMEM((STEPS + 1, 8, PIX), F32),
            pltpu.VMEM((STEPS, 8, C), F32),
            pltpu.VMEM((STEPS, C, PIX), BF16),
            pltpu.VMEM((STEPS, C, PIX), BF16),
            pltpu.VMEM((C, PIX), BF16),
            pltpu.VMEM((80, PIX), F32),
            pltpu.VMEM((C, 80), F32),
            pltpu.VMEM((C, 128), F32),
        ],
        name="chain",
    )(*[near(x) for x in (recv, w_fwd, w_bwd, emb, rows, cols, spread, means)], steps)


def finish_kernel(own, other, w_out_t, path, grad):
    index = position()[1]
    core, turn = index % 2, (128 - SIDE * (index // 4)) % 128
    for r in range(2):
        k = 36 + 4 * r
        mine = jnp.where(core == 0, own[k : k + 4, 0:128], own[k + 8 : k + 12, 0:128])
        theirs = jnp.where(core == 0, other[k : k + 4, 0:128], other[k + 8 : k + 12, 0:128])
        first = jnp.where(core == 0, mine, theirs)
        second = jnp.where(core == 0, theirs, mine)
        for m, x in enumerate((first, second)):
            x = pltpu.roll(x, turn, 1)
            for c in range(CH):
                path[0, m, c, r : r + 1] = x[c : c + 1, 0:SIDE]
    width = grad.shape[1]
    weights = jnp.concatenate([w_out_t[...], jnp.zeros((CH, 384 - C), F32)], axis=1)
    weights = pltpu.roll(weights, (384 - width * index) % 384, 1)[:, :128]
    w_head = weights.astype(BF16).astype(F32)
    left = jnp.concatenate([w_head, w_head, weights - w_head, weights * 0.0], axis=0)
    left = left.T[:24].astype(BF16)
    both = own[0:36] + other[0:36]
    head = both.astype(BF16).astype(F32)
    tail = both - head
    for k in range(9):
        at = slice(4 * k, 4 * k + 4)
        right = jnp.concatenate([head[at], tail[at], head[at], tail[at]], axis=0)
        grad[k] = dot(left, right.astype(BF16))[:width]


def finish(own, other, w_out_t, width):
    vmem = pl.BlockSpec(memory_space=pltpu.VMEM)
    return pl.pallas_call(
        finish_kernel,
        out_shape=(
            jax.ShapeDtypeStruct((1, 2, CH, 2, SIDE), F32),
            jax.ShapeDtypeStruct((9, width, C), F32),
        ),
        in_specs=[vmem] * 3,
        out_specs=(vmem, vmem),
        name="finish",
    )(own, other, w_out_t)


def local(noise, target, timesteps, w_in, gn_gain, w_time1, w_time2, w_conv, w_out):
    count = lax.axis_size("tensor")
    recv = lax.all_to_all(near(pack(noise, target)), "tensor", 0, 0, tiled=True)
    w_out_t = w_out.T
    made = prepare(timesteps, w_out_t, w_in, gn_gain, w_time1, w_time2.T, w_conv)
    own = chain(recv, *made)
    other = lax.ppermute(own, "tensor", [(i, i ^ 1) for i in range(count)])
    path, grad = finish(near(own), near(other), near(w_out_t), C // count)
    return path, jnp.swapaxes(grad, 1, 2)


def solution(mesh):
    placed = (
        P(None, None, "tensor", None),
        P(None, None, "tensor", None),
        P(),
        P(),
        P(),
        P(),
        P(),
        P(),
        P(),
    )
    return jax.shard_map(
        local,
        mesh=mesh,
        in_specs=placed,
        out_specs=(P("section", None, None, "tensor", None), P(None, None, "tensor")),
        check_vma=False,
    )
```

```python
import math

import jax
import jax.numpy as jnp
import numpy as np
from jax import lax
from jax.experimental import pallas as pl
from jax.experimental.pallas import tpu as pltpu
from jax.sharding import PartitionSpec as P


GROUPS = 32
STEPS = 16
CH = 4
C = 320
SIDE = 32
PIX = SIDE * SIDE
TILE = 256
F32 = jnp.float32
BF16 = jnp.bfloat16
EPS = 1e-05


def schedule_tables():
    grid = np.arange(1000, dtype=np.float64)
    low, high = math.sqrt(0.00085), math.sqrt(0.012)
    bar = np.cumprod(1.0 - (low + grid * ((high - low) / 999.0)) ** 2)
    table = np.zeros((3, 1024), np.float32)
    table[0, :1000] = np.sqrt(bar)
    table[1, :1000] = 1.0 / np.sqrt(bar)
    table[2, :1000] = np.sqrt(1.0 - bar)
    return table


def split(x, parts):
    out = []
    for _ in range(parts):
        head = x.astype(BF16)
        out.append(head)
        x = x - head.astype(F32)
    return out


def dot(a, b, dims=((1,), (0,)), precision=None):
    return lax.dot_general(a, b, (dims, ((), ())), precision=precision, preferred_element_type=F32)


NT = ((1,), (1,))


def rolled(x, shift, axis):
    return pltpu.roll(x, shift % x.shape[axis], axis)


def doubled(x):
    return jnp.concatenate([x, x], axis=0)


def row_index(shape):
    return lax.broadcasted_iota(jnp.int32, shape, 0)


def position():
    return lax.axis_index("section"), lax.axis_index("tensor")


def wave_tables():
    half = C // 2
    f = np.exp(-math.log(10000.0) * np.arange(half, dtype=np.float64) / half)
    step = np.arange(32, dtype=np.float64)[:, None]
    big, small = 32.0 * step * f, step * f
    both = lambda a, b: np.concatenate([a, b], axis=1)
    return np.stack(
        [
            both(np.cos(big), np.sin(big)),
            both(-np.sin(big), np.cos(big)),
            both(np.cos(small), np.cos(small)),
            both(np.sin(small), np.sin(small)),
        ]
    ).astype(np.float32)


def near(x):
    return pltpu.with_memory_space_constraint(x, pltpu.VMEM)


def pack_kernel(noise, target, packed):
    for m in range(2):
        parts = [x[m, :, r, :] for x in (noise, target) for r in range(2)]
        tile = jnp.concatenate(parts, axis=1)
        for j in range(8):
            packed[2 * j + m] = tile


def pack(noise, target):
    vmem = pl.BlockSpec(memory_space=pltpu.VMEM)
    return pl.pallas_call(
        pack_kernel,
        out_shape=pltpu.VMEM((16, CH, 128), F32),
        in_specs=[vmem] * 2,
        out_specs=vmem,
        name="pack",
    )(noise, target)


def regrouped(x, buffer):
    buffer[...] = x
    size = C // GROUPS
    return jnp.concatenate([buffer[pl.ds(k, GROUPS, stride=size), :] for k in range(size)], axis=0)


def two(x):
    head = x.astype(BF16)
    return head, (x - head.astype(F32)).astype(BF16)


def stacked(a, b):
    return jnp.concatenate([a.astype(F32), b.astype(F32)], axis=0).astype(BF16)


def prepare_kernel(
    times, tables, waves, w_out_t, w_in, gain, w1_hbm, w2t_hbm, conv_hbm,
    w_fwd, w_bwd, emb, rows, cols, spread, means, steps, w1, w2t, conv, buffer, sems,
):
    copies = [pltpu.make_async_copy(conv_hbm.at[k], conv.at[k], sems.at[k]) for k in range(9)]
    copies.append(pltpu.make_async_copy(w1_hbm, w1, sems.at[9]))
    copies.append(pltpu.make_async_copy(w2t_hbm, w2t, sems.at[10]))
    for c in copies:
        c.start()
    for s in range(STEPS):
        now = times[s]
        last = s == STEPS - 1
        root = 1.0 if last else tables[0, times[s + 1]]
        rest = 0.0 if last else tables[2, times[s + 1]]
        keep = root * tables[1, now]
        steps[0, s] = keep
        steps[1, s] = rest - keep * tables[2, now]
    out8 = doubled(w_out_t[...])
    in8 = doubled(w_in[...])
    first = row_index((8, C)) < CH
    next1, next2 = rolled(in8, -1, 0), rolled(in8, -2, 0)
    top = jnp.where(first, in8, in8 * in8)
    low = in8 * jnp.where(first, 2.0 * next1, next2)
    group = lambda axis: lax.broadcasted_iota(jnp.int32, (C, C), axis) * 6554 >> 16
    member = jnp.where(group(0) == group(1), 1.0, 0.0).astype(BF16)
    both = jnp.concatenate([top, low], axis=0)
    p1, p2, p3 = [p.astype(F32) for p in split(both, 3)]
    sums = dot(jnp.concatenate([p1, p2, p3], axis=0).astype(BF16), member)
    sums = (sums[0:16] + sums[16:32] + sums[32:48]) * (1.0 / (PIX * (C // GROUPS)))
    half_gain = 0.5 * gain[...].reshape(1, C)
    place8 = row_index((8, C))
    folded = jnp.where(place8 < CH, in8, jnp.where(place8 == CH, 1.0, 0.0)) * half_gain
    gain8 = jnp.broadcast_to(half_gain, (8, C))
    table = jnp.concatenate(
        [folded, folded, folded, in8, sums, gain8, jnp.zeros((72, C), F32)], axis=0
    )
    ordered = regrouped(table.T, buffer)
    spread[...] = ordered
    for j in range(16):
        means[j] = jnp.broadcast_to(ordered[0:GROUPS, 32 + j : 33 + j], (GROUPS, 128))
    turned = ordered.T
    for c in range(CH):
        rows[16 * (c + 1) : 16 * (c + 2)] = turned[32:48] * turned[24 + c : 25 + c]
    rows[0:16] = turned[32:48]
    rows[80:88] = turned[48:56]
    rows[88:96] = turned[24:32]
    for j in range(CH):
        ahead = jnp.sum(out8 * rolled(in8, -j, 0), axis=1, keepdims=True)
        back = jnp.sum(rolled(out8, -j, 0) * in8, axis=1, keepdims=True)
        cols[j] = jnp.broadcast_to(ahead, (8, 128))
        cols[CH + j] = jnp.broadcast_to(back, (8, 128))
    repeated = jnp.concatenate([out8] * 16, axis=0).T
    lane = lax.broadcasted_iota(jnp.int32, (C, 128), 1)
    r_head, r_tail = two(repeated)
    r_head, r_tail = r_head.astype(F32), r_tail.astype(F32)
    acc = jnp.zeros((C, 256), F32)
    for k in range(9):
        copies[k].wait()
    for k in range(9):
        at = lane // 8 == k
        right = jnp.concatenate([jnp.where(at, r_head, 0.0), jnp.where(at, r_tail, 0.0)], axis=1)
        acc = acc + dot(conv[k], right.astype(BF16))
    full = regrouped(acc[:, :128] + acc[:, 128:], buffer)
    head = full.astype(BF16).astype(F32)
    tail = full - head
    w_bwd[...] = jnp.concatenate([head[:, :80], tail[:, :80]], axis=1).astype(BF16)
    w_fwd[...] = jnp.where(lane % 8 < CH, head, tail).T[:80].astype(BF16)
    feats = []
    for s in range(STEPS):
        t = times[s]
        a, b = t >> 5, t & 31
        feats.append(
            waves[0, pl.ds(a, 1)] * waves[2, pl.ds(b, 1)]
            + waves[1, pl.ds(a, 1)] * waves[3, pl.ds(b, 1)]
        )
    f_head, f_tail = two(jnp.concatenate(feats, axis=0))
    o_head, o_tail = two(out8)
    copies[9].wait()
    copies[10].wait()
    w_head, w_tail = two(w1[...])
    z = dot(stacked(f_head, f_tail), w_head)
    z = 0.5 * (z[:STEPS] + z[STEPS:] + dot(f_head, w_tail))
    hidden = z + z * jnp.tanh(z)
    w_head, w_tail = two(w2t[...])
    y = dot(stacked(o_head, o_tail), w_head)
    y = y[0:8] + y[8:16] + dot(o_head, w_tail)
    y_head, y_tail = two(y)
    h_head, h_tail = two(hidden)
    x = dot(stacked(y_head, y_tail), h_head, NT)
    shift = x[0:8] + x[8:16] + dot(y_head, h_tail, NT)
    for s in range(STEPS):
        emb[s] = jnp.broadcast_to(shift[:, s : s + 1], (8, 128))


def prepare(times, w_out_t, w_in, gain, w1, w2t, w_conv):
    smem = pl.BlockSpec(memory_space=pltpu.SMEM)
    vmem = pl.BlockSpec(memory_space=pltpu.VMEM)
    hbm = pl.BlockSpec(memory_space=pl.ANY)
    return pl.pallas_call(
        prepare_kernel,
        out_shape=(
            pltpu.VMEM((80, C), BF16),
            pltpu.VMEM((C, 160), BF16),
            pltpu.VMEM((STEPS, 8, 128), F32),
            pltpu.VMEM((96, C), F32),
            pltpu.VMEM((8, 8, 128), F32),
            pltpu.VMEM((C, 128), F32),
            pltpu.VMEM((16, GROUPS, 128), F32),
            pltpu.SMEM((2, STEPS), F32),
        ),
        in_specs=[smem] * 2 + [vmem] * 4 + [hbm] * 3,
        out_specs=(vmem,) * 7 + (smem,),
        scratch_shapes=[
            pltpu.VMEM(w1.shape, F32),
            pltpu.VMEM(w2t.shape, F32),
            pltpu.VMEM(w_conv.shape, BF16),
            pltpu.VMEM((C, 128), F32),
            pltpu.SemaphoreType.DMA((11,)),
        ],
        name="prepare",
    )(times, jnp.asarray(schedule_tables()), jnp.asarray(wave_tables()), w_out_t, w_in, gain, w1, w2t, w_conv)


def repeated(step, state, group):
    def several(i, state):
        for k in range(group):
            state = step(group * i + k, state)
        return state

    return lax.fori_loop(0, STEPS // group, several, state)


def wide(col):
    return jnp.concatenate([col] * (PIX // 128), axis=1)


def chain_kernel(
    recv, w_fwd, w_bwd, emb, rows, cols, spread, means, steps,
    sent, lat, stat, act, half, slope, taps, total, ordered,
):
    section, index = position()
    rid = row_index((8, PIX))
    upper = rid < CH
    lane = lax.broadcasted_iota(jnp.int32, (8, 128), 1)
    column = lane % SIDE
    col_ok = {1: column > 0, 0: None, -1: column < SIDE - 1}
    low_ok, high_ok = lane >= SIDE, lane < 128 - SIDE
    supper = row_index((8, C)) < CH
    glane = lax.broadcasted_iota(jnp.int32, (GROUPS, 128), 1)
    slane = lax.broadcasted_iota(jnp.int32, (C, 128), 1)
    in8 = rows[88:96]
    half_gain = rows[80:81]

    def piece(x, v):
        return x[:, 128 * v : 128 * v + 128]

    def moved(x, d):
        return x if d == 0 else jnp.where(col_ok[d], rolled(x, d, 1), 0.0)

    def moved_low(x, d):
        y = rolled(x, SIDE + d, 1)
        return jnp.where(low_ok if d == 0 else low_ok & col_ok[d], y, 0.0)

    def moved_high(x, d):
        y = rolled(x, d - SIDE, 1)
        return jnp.where(high_ok if d == 0 else high_ok & col_ok[d], y, 0.0)

    got = [recv[i] for i in range(16)]

    def gathered(base):
        parts = []
        for v in range(8):
            at = base + SIDE * (v % 2)
            parts.extend(got[(8 * q + v) // 2][:, at : at + SIDE] for q in range(4))
        return doubled(jnp.concatenate(parts, axis=1))

    latent0, target8 = gathered(0), gathered(2 * SIDE)

    def coefs(s):
        return steps[0, s], steps[1, s]

    def forward(s, l8):
        keep, nc = coefs(s)
        lat[s] = l8
        r1, r2, r3 = rolled(l8, -1, 0), rolled(l8, -2, 0), rolled(l8, -3, 0)
        x0 = jnp.where(upper, l8, l8 * l8)
        x1 = l8 * jnp.where(upper, r1, r2)
        m0 = jnp.sum(x0, axis=1, keepdims=True)
        m1 = jnp.sum(x1, axis=1, keepdims=True)
        p0 = rows[0:8] * m0
        p1 = rows[8:16] * m1
        avg = jnp.sum(jnp.where(supper, p0, 0.0), axis=0, keepdims=True)
        sq = jnp.sum(jnp.where(supper, 0.0, p0) + p1, axis=0, keepdims=True)
        rstd = lax.rsqrt(sq - avg * avg + EPS)
        scale = rstd * half_gain
        stat[s, 0:1] = avg
        stat[s, 1:2] = rstd
        stat[s, 2:3] = scale
        k0, k1 = jnp.broadcast_to(m0, (8, 128)), jnp.broadcast_to(m1, (8, 128))
        terms = [means[j] * k0[j : j + 1] for j in range(8)]
        terms += [means[8 + j] * k1[j : j + 1] for j in range(8)]
        gavg = (terms[0] + terms[1]) + (terms[2] + terms[3])
        gsq = ((terms[4] + terms[5]) + (terms[6] + terms[7])) + (
            ((terms[8] + terms[9]) + (terms[10] + terms[11]))
            + ((terms[12] + terms[13]) + (terms[14] + terms[15]))
        )
        factor = lax.rsqrt(gsq - gavg * gavg + EPS)
        factor = jnp.where(glane % 8 == CH, -gavg * factor, factor)
        wz = spread[...] * jnp.concatenate([factor] * (C // GROUPS), axis=0)
        a = wz.astype(BF16).astype(F32)
        wzs = jnp.where(slane >= 16, wz - a, a).astype(BF16)[:, :24]
        hom = jnp.where(upper, l8, jnp.where(rid == CH, 1.0, 0.0))
        d = hom.astype(BF16).astype(F32)
        ls = jnp.concatenate([d, hom - d, d], axis=0).astype(BF16)
        linear = (
            wide(cols[0]) * l8 + wide(cols[1]) * r1 + wide(cols[2]) * r2 + wide(cols[3]) * r3
        )
        linear = keep * l8 + nc * (linear + wide(emb[s]))
        tiles = [slice(j * TILE, (j + 1) * TILE) for j in range(PIX // TILE)]
        hs = [dot(wzs, ls[:, at]) for at in tiles]
        for at, h in zip(tiles, hs):
            t = jnp.tanh(h)
            u = h * t
            narrow = (h + u).astype(BF16)
            act[s, :, at] = narrow
            taps[:, at] = dot(w_fwd[...], narrow)
            half[s, :, at] = t.astype(BF16)

        def tap(dy, dx, v):
            k = 8 * (3 * dy + dx)
            return taps[k : k + 8, 128 * v : 128 * v + 128]

        out = []
        for v in range(8):
            conv = None
            for dx in (1, 0, 2):
                d = 1 - dx
                part = tap(1, dx, v)
                if v > 0:
                    part = part + tap(0, dx, v - 1)
                if v < 7:
                    part = part + tap(2, dx, v + 1)
                part = moved(part, d)
                conv = part if conv is None else conv + part
                if v == 0:
                    conv = conv + moved_low(tap(0, dx, 7), d)
                if v == 7:
                    conv = conv + moved_high(tap(2, dx, 0), d)
            conv = conv + rolled(conv, 4, 0)
            out.append(piece(linear, v) + nc * conv)
        return jnp.concatenate(out, axis=1)

    final = repeated(forward, latent0, 4)
    lat[STEPS] = final
    total[...] = jnp.zeros_like(total)
    erow = row_index((16, C)) < CH

    def backward(i, adj):
        s = STEPS - 1 - i
        keep, nc = coefs(s)
        l8 = lat[s]
        avg, rstd, scale = stat[s, 0:1], stat[s, 1:2], stat[s, 2:3]
        ng = nc * adj
        head = ng.astype(BF16).astype(F32)
        x = jnp.where(upper, head, ng - head)
        first, last = piece(x, 0), piece(x, 7)
        above, same, below = [], [], []
        for d in (-1, 0, 1):
            ys = [moved(piece(x, v), d) for v in range(8)]
            same.append(jnp.concatenate(ys, axis=1))
            above.append(jnp.concatenate(ys[1:] + [moved_high(first, d)], axis=1))
            below.append(jnp.concatenate([moved_low(last, d)] + ys[:7], axis=1))
        pad = jnp.zeros_like(x)
        a80 = jnp.concatenate(above + same + below + [pad], axis=0).astype(BF16)
        col = jnp.concatenate([a80, a80], axis=0)
        ws = in8 * scale
        whead = ws.astype(BF16).astype(F32)
        wd = jnp.where(supper, whead, ws - whead)
        q = (-0.5 * rstd * rstd * rstd) * half_gain
        qa = q * avg
        per = jnp.where(erow, -2.0 * qa, q)
        one = jnp.where(erow, 2.0 * qa * avg - scale, -qa)
        phi = [rows[16 * (c + 1) : 16 * (c + 2)] * per for c in range(CH)]
        phi = jnp.concatenate(phi + [rows[0:16] * one, wd, jnp.zeros_like(wd)], axis=0).astype(BF16)
        tiles = [slice(j * TILE, (j + 1) * TILE) for j in range(PIX // TILE)]
        for at in tiles:
            t = half[s, :, at]
            slope[:, at] = (1 + t) + act[s, :, at] * (1 - t)
        gs = [dot(w_bwd[...], col[:, at]) for at in tiles]
        outs = []
        for at, g in zip(tiles, gs):
            outs.append(dot(phi, g.astype(BF16) * slope[:, at]))
        total[...] += dot(act[s], a80, NT)
        z = jnp.concatenate(outs, axis=1)
        dl = z[80:88]
        dl = dl + rolled(dl, 4, 0)
        acc0, acc1 = z[64:72], z[72:80]
        for c in range(CH):
            lc = l8[c : c + 1]
            acc0 = acc0 + z[16 * c : 16 * c + 8] * lc
            acc1 = acc1 + z[16 * c + 8 : 16 * c + 16] * lc
        c0 = jnp.sum(acc0, axis=1, keepdims=True)
        c1 = jnp.sum(acc1, axis=1, keepdims=True)
        c0 = jnp.broadcast_to(c0, (8, 128))
        c1 = jnp.broadcast_to(c1, (8, 128))
        up8 = upper[:, :128]
        c0r, c1r = rolled(c0, 4, 0), rolled(c1, 4, 0)
        dm = jnp.where(up8, c0, c0r)
        d0 = 2.0 * jnp.where(up8, c0r, c0)
        d1 = jnp.where(up8, c1, c1r)
        d3 = rolled(d1, 1, 0)
        d2 = jnp.where(up8, c1r, c1)
        d2 = d2 + rolled(d2, 2, 0)
        r1, r2, r3 = rolled(l8, -1, 0), rolled(l8, -2, 0), rolled(l8, -3, 0)
        a1, a2, a3 = rolled(adj, -1, 0), rolled(adj, -2, 0), rolled(adj, -3, 0)
        linear = (
            wide(cols[4]) * adj + wide(cols[5]) * a1 + wide(cols[6]) * a2 + wide(cols[7]) * a3
        )
        linear = keep * adj + nc * linear + dl
        stats = wide(dm) + wide(d0) * l8 + wide(d1) * r1 + wide(d2) * r2 + wide(d3) * r3
        return linear + stats

    repeated(backward, final - target8, 8)
    size = C // GROUPS
    for k in range(size):
        ordered[pl.ds(k, GROUPS, stride=size), 0:80] = total[GROUPS * k : GROUPS * k + GROUPS]
    turned = ordered[:, 0:80].T
    for k in range(9):
        part = turned[8 * k : 8 * k + 8]
        part = part + rolled(part, 4, 0)
        sent[4 * k : 4 * k + 4] = part[0:4]
    mine = lat[section + 1, :, pl.ds(pl.multiple_of(index % 4 // 2 * 512, 512), 512)]
    blank = jnp.zeros((4, C - 128), F32)
    for v in range(4):
        sent[36 + 4 * v : 40 + 4 * v] = jnp.concatenate([piece(mine, v)[0:4], blank], axis=1)


def chain(recv, w_fwd, w_bwd, emb, rows, cols, spread, means, steps):
    smem = pl.BlockSpec(memory_space=pltpu.SMEM)
    vmem = pl.BlockSpec(memory_space=pltpu.VMEM)
    return pl.pallas_call(
        chain_kernel,
        out_shape=pltpu.VMEM((56, C), F32),
        in_specs=[vmem] * 8 + [smem],
        out_specs=vmem,
        scratch_shapes=[
            pltpu.VMEM((STEPS + 1, 8, PIX), F32),
            pltpu.VMEM((STEPS, 8, C), F32),
            pltpu.VMEM((STEPS, C, PIX), BF16),
            pltpu.VMEM((STEPS, C, PIX), BF16),
            pltpu.VMEM((C, PIX), BF16),
            pltpu.VMEM((80, PIX), F32),
            pltpu.VMEM((C, 80), F32),
            pltpu.VMEM((C, 128), F32),
        ],
        name="chain",
    )(*[near(x) for x in (recv, w_fwd, w_bwd, emb, rows, cols, spread, means)], steps)


def finish_kernel(own, other, w_out_t, path, grad):
    index = position()[1]
    core, turn = index % 2, (128 - SIDE * (index // 4)) % 128
    for r in range(2):
        k = 36 + 4 * r
        mine = jnp.where(core == 0, own[k : k + 4, 0:128], own[k + 8 : k + 12, 0:128])
        theirs = jnp.where(core == 0, other[k : k + 4, 0:128], other[k + 8 : k + 12, 0:128])
        first = jnp.where(core == 0, mine, theirs)
        second = jnp.where(core == 0, theirs, mine)
        for m, x in enumerate((first, second)):
            x = pltpu.roll(x, turn, 1)
            for c in range(CH):
                path[0, m, c, r : r + 1] = x[c : c + 1, 0:SIDE]
    width = grad.shape[1]
    weights = jnp.concatenate([w_out_t[...], jnp.zeros((CH, 384 - C), F32)], axis=1)
    weights = pltpu.roll(weights, (384 - width * index) % 384, 1)[:, :128]
    w_head = weights.astype(BF16).astype(F32)
    left = jnp.concatenate([w_head, w_head, weights - w_head, weights * 0.0], axis=0)
    left = left.T[:24].astype(BF16)
    both = own[0:36] + other[0:36]
    head = both.astype(BF16).astype(F32)
    tail = both - head
    for k in range(9):
        at = slice(4 * k, 4 * k + 4)
        right = jnp.concatenate([head[at], tail[at], head[at], tail[at]], axis=0)
        grad[k] = dot(left, right.astype(BF16))[:width]


def finish(own, other, w_out_t, width):
    vmem = pl.BlockSpec(memory_space=pltpu.VMEM)
    return pl.pallas_call(
        finish_kernel,
        out_shape=(
            jax.ShapeDtypeStruct((1, 2, CH, 2, SIDE), F32),
            jax.ShapeDtypeStruct((9, width, C), F32),
        ),
        in_specs=[vmem] * 3,
        out_specs=(vmem, vmem),
        name="finish",
    )(own, other, w_out_t)


def local(noise, target, timesteps, w_in, gn_gain, w_time1, w_time2, w_conv, w_out):
    count = lax.axis_size("tensor")
    recv = lax.all_to_all(near(pack(noise, target)), "tensor", 0, 0, tiled=True)
    w_out_t = w_out.T
    made = prepare(timesteps, w_out_t, w_in, gn_gain, w_time1, w_time2.T, w_conv)
    own = chain(recv, *made)
    other = lax.ppermute(own, "tensor", [(i, i ^ 1) for i in range(count)])
    path, grad = finish(near(own), near(other), near(w_out_t), C // count)
    return path, jnp.swapaxes(grad, 1, 2)


def solution(mesh):
    placed = (
        P(None, None, "tensor", None),
        P(None, None, "tensor", None),
        P(),
        P(),
        P(),
        P(),
        P(),
        P(),
        P(),
    )
    return jax.shard_map(
        local,
        mesh=mesh,
        in_specs=placed,
        out_specs=(P("section", None, None, "tensor", None), P(None, None, "tensor")),
        check_vma=False,
    )
```
